256 devices in a mesh: blk: 16 (over x_lo, z), tgt: 16 (over y, x_hi, core).
Axes of the slice: x: 4 (x_hi: 2, x_lo: 2; x = x_hi * 2 + x_lo), y: 4, z: 8, core: 2. Of those that a mesh axis runs over, the one named last changes fastest.
Arguments:
- sources: float32 [16384, 128], P('blk'), may hold values from -0.5 to 0.5, as said below
- targets: float32 [65536, 128], P(('blk', 'tgt')), may hold values from -0.5 to 0.5, as said below
- duals_init: float32 [65536], P(('blk', 'tgt')), may hold values from -1.5 to 1.5
Outputs:
- source_duals: float32 [16384], P('blk')
- target_duals: float32 [65536], P(('blk', 'tgt'))
The draws below stay inside these ranges and needn't reach their ends.
Inputs may be any that keep to these rules, and one draw needn't show every extreme that they name: `sources`: coordinates of the source points. `targets`: coordinates of the target points.
All inputs are finite; a program needn't handle non-finite values.
Results may differ from the reference program's by a relative error of at most 0.0001.
Values sent between devices are 32-bit elements; how exact they have to be, the bound alone decides.
A program may use at most 64 MiB of HBM per device.

```python
import jax
import jax.numpy as jnp
from jax import lax

D = 128
ROWS_DEV = 1024
TGT_DEV = 256
ITERS = 2
N_SRC = 16384
N_DST = 65536


def common_offset(key):
    inner = jax.random.fold_in(key, 11)
    size_key, sign_key = jax.random.split(inner)
    magnitude = jax.random.uniform(size_key, (D,), jnp.float32, 0.15, 0.25)
    signs = jnp.where(jax.random.bernoulli(sign_key, 0.5, (D,)), 1.0, -1.0)
    return magnitude * signs


def cloud_points(key, salt, count):
    offset = common_offset(key)
    inner = jax.random.fold_in(key, salt)
    base_key, pick_key, sign_key, size_key = jax.random.split(inner, 4)
    base = 0.0625 * jax.random.truncated_normal(base_key, -6.0, 6.0, (count, D), jnp.float32)
    chosen = jax.random.randint(pick_key, (count,), 0, 48) == 0
    signs = jnp.where(jax.random.bernoulli(sign_key, 0.5, (count, D)), 1.0, -1.0)
    strength = jax.random.uniform(size_key, (count, 1), jnp.float32, 0.6, 1.0)
    far_part = 0.45 * strength * signs
    local = jnp.where(chosen[:, None], far_part, base)
    return jnp.clip(offset[None, :] + local, -0.5, 0.5)


def draw_sources(key, part):
    return cloud_points(key, 3, N_SRC)


def draw_targets(key, part):
    return cloud_points(key, 5, N_DST)


def steps_of(stream_key, shape, cuts, smallest, high):
    loudness, own = 1.0, jax.random.fold_in(stream_key, 6)
    for dim, shards_of in cuts:
        draws = jnp.exp(jax.random.uniform(jax.random.fold_in(own, dim), (shards_of,), jnp.float32, smallest / len(cuts), high / len(cuts)))
        loudness = loudness * jnp.repeat(draws, shape[dim] // shards_of).reshape([-1 if axis == dim else 1 for axis in range(len(shape))])
    return loudness


def scatter_about(own_key, extent, deviation, bound, pieces=(), held_as=jnp.bfloat16):
    entries = deviation * jax.random.normal(own_key, extent, jnp.float32)
    if pieces:
        entries = entries * steps_of(own_key, extent, pieces, -0.22, 0.18)
    return jnp.clip(entries, -bound, bound).astype(held_as)


def setup_inputs(seed: int = 0) -> dict:
    arg_keys = jax.random.split(jax.random.key(seed), 4)
    sources = draw_sources(jax.random.fold_in(arg_keys[3], 71), 0)
    targets = draw_targets(jax.random.fold_in(arg_keys[3], 71), 0)
    duals_init = scatter_about(arg_keys[2], (N_DST,), 0.3, 1.5, ((0, 256),), jnp.float32)
    return {"sources": sources, "targets": targets, "duals_init": duals_init}


EPS = 0.05


def block_lse(left_blk, left_norm, right, right_norm, right_pots):
    cross = jnp.dot(left_blk, right.T, preferred_element_type=jnp.float32, precision=lax.Precision.HIGHEST)
    cost_tile = left_norm[:, None] + right_norm[None, :] - 2.0 * cross
    scores = (right_pots[None, :] - cost_tile) / EPS
    maxima = jnp.max(scores, axis=1)
    return maxima + jnp.log(jnp.sum(jnp.exp(scores - maxima[:, None]), axis=1))


def half_step(left, left_norm, right, right_norm, right_pots, block):
    count = left.shape[0] // block
    left_blocks = left.reshape(count, block, left.shape[1])
    norm_blocks = left_norm.reshape(count, block)
    result = lax.map(lambda pair: block_lse(pair[0], pair[1], right, right_norm, right_pots), (left_blocks, norm_blocks))
    return EPS * (-jnp.log(jnp.float32(right.shape[0]))) - EPS * result.reshape(-1)


def reference(sources, targets, duals_init):
    src_norm = jnp.sum(sources * sources, axis=1)
    dst_norm = jnp.sum(targets * targets, axis=1)
    target_pots = duals_init
    source_pots = jnp.zeros_like(src_norm)
    for repeat in range(ITERS):
        source_pots = half_step(sources, src_norm, targets, dst_norm, target_pots, ROWS_DEV)
        target_pots = half_step(targets, dst_norm, sources, src_norm, source_pots, TGT_DEV)
    return source_pots, target_pots
```

```python
import functools
import math

import jax
import jax.numpy as jnp
from jax import lax
from jax.experimental import pallas as pl
from jax.experimental.pallas import tpu as pltpu
from jax.sharding import PartitionSpec as P

EPS = 0.05
LOG2E = math.log2(math.e)
SCALE = LOG2E / EPS
MESH = pl.DeviceIdType.MESH
NZ = 8
NP = 16
ROWS = 1024
COLS = 256
BLOCKS = 16
HEAD = 8
D = 128
LANES = 128
CHUNK = 128
CUTS = ((0, HEAD + CHUNK), (HEAD + CHUNK, CHUNK))
F32 = jnp.float32


def lse2(parts):
    high = functools.reduce(jnp.maximum, parts)
    total = functools.reduce(jnp.add, [jnp.exp2(p - high) for p in parts])
    return high + jnp.log2(total)


def kernel(
    log_src, log_dst,
    src_ref, tgt_ref, g0_ref, f_ref, g_ref,
    tile, blocks, rows_in, lhs, acc, wide,
    row_stat, col_stat, beta, delta, weight,
    row_buf, pair_buf, z_buf, own_buf, fin_buf, f_own, f_pair,
    ring_send, ring_recv, d2d_send, d2d_recv, x_send, x_recv,
    row_send, row_recv, z_send, z_recv, pair_send, pair_recv,
):
    blk, tgt = lax.axis_index("blk"), lax.axis_index("tgt")
    x_lo, z = blk // NZ, lax.rem(blk, NZ)
    core, x_hi, y = lax.rem(tgt, 2), lax.rem(tgt // 2, 2), tgt // 4
    pair = (blk, tgt + 1 - 2 * core)
    me = x_lo * 8 + tgt // 2

    def on_plane(q):
        return (q // 8) * NZ + z, lax.rem(q, 8) * 2 + core

    def on_ring(other):
        return x_lo * NZ + other, tgt

    def beside(step):
        x = lax.rem(2 * x_hi + x_lo + step + 4, 4)
        return lax.rem(x, 2) * NZ + z, y * 4 + (x // 2) * 2 + x_lo

    swaps = core != x_lo
    left, right = beside(-1), beside(1)

    barrier = pltpu.get_barrier_semaphore()
    for k in range(1, NP):
        pl.semaphore_signal(barrier, inc=1, device_id=on_plane(lax.rem(me + k, NP)), device_id_type=MESH)
    for k in range(1, NZ):
        pl.semaphore_signal(barrier, inc=1, device_id=on_ring(lax.rem(z + k, NZ)), device_id_type=MESH)
    pl.semaphore_signal(barrier, inc=1, device_id=pair, device_id_type=MESH)

    @pl.when(swaps)
    def _():
        for there in (left, right):
            pl.semaphore_signal(barrier, inc=1, device_id=there, device_id_type=MESH)

    own = core * NZ + z
    mine = tgt_ref[...]
    for half in range(2):
        part = mine[half * LANES : (half + 1) * LANES, :]
        norm = jnp.sum((part * part).T, axis=0, keepdims=True)
        blocks[own, half : half + 1, :] = SCALE * (g0_ref[half : half + 1, :] - norm)
    blocks[own, HEAD:, :] = mine

    pl.semaphore_wait(barrier, NP - 1 + NZ - 1 + 1 + 2 * swaps.astype(jnp.int32))

    def copy(src, dst, send, recv, where):
        return pltpu.make_async_remote_copy(
            src_ref=src, dst_ref=dst, send_sem=send, recv_sem=recv, device_id=where, device_id_type=MESH
        )

    def piece(b, k):
        start, size = CUTS[k]
        return blocks.at[b, pl.ds(start, size), :]

    def ring_copy(way, step, k, b):
        to = on_ring(lax.rem(z + (1 if way == 0 else NZ - 1), NZ))
        slot = 2 * (step - 1) + (k if step < 4 else 0)
        return copy(piece(b, k), piece(b, k), ring_send.at[way, slot], ring_recv.at[way, slot], to)

    def pair_copy(b, k):
        at = lax.rem(b, NZ) * 2 + k
        return copy(piece(b, k), piece(b, k), d2d_send.at[at], d2d_recv.at[at], pair)

    def swap_copy(side):
        at = pl.ds(side * (ROWS // 2), ROWS // 2)
        return copy(src_ref.at[at, :], rows_in.at[at, :], x_send.at[side], x_recv.at[side], (left, right)[side])

    for k in range(2):
        for way in range(2):
            ring_copy(way, 1, k, own).start()

    @pl.when(swaps)
    def _():
        for side in range(2):
            swap_copy(side).start()

    for k in range(2):
        pair_copy(own, k).start()

    @pl.when(jnp.logical_not(swaps))
    def _():
        rows_in[...] = src_ref[...]

    def origin(way, step):
        return lax.rem(z + (NZ - step if way == 0 else step), NZ)

    def receive(step, k):
        for way in range(2):
            if step == 4 and k != way:
                continue
            b = core * NZ + origin(way, step)
            ring_copy(way, step, k, b).wait_recv()
            if step < 3 or (step == 3 and k == way):
                ring_copy(way, step + 1, k, b).start()
            pair_copy(b, k).start()

    def prepare():
        @pl.when(swaps)
        def _():
            for side in range(2):
                swap_copy(side).wait()

        for r in range(ROWS // LANES):
            rows = rows_in[r * LANES : (r + 1) * LANES, :] * (2 * SCALE)
            high = rows.astype(jnp.bfloat16)
            low = (rows - high.astype(F32)).astype(jnp.bfloat16)
            lhs[r * LANES : (r + 1) * LANES, :] = jnp.concatenate([high, low, high, low], axis=1)
        acc[...] = jnp.full_like(acc, -jnp.inf)

    def scores(b):
        t = blocks[b, HEAD:, :]
        high = t.astype(jnp.bfloat16)
        low = (t - high.astype(F32)).astype(jnp.bfloat16)
        rhs = jnp.concatenate([high, high, low, low], axis=1)
        head = jnp.concatenate([blocks[b, 0:1, :], blocks[b, 1:2, :]], axis=1)
        out = lax.dot_general(lhs[...], rhs, (((1,), (1,)), ((), ())), preferred_element_type=F32) + head
        tile[b] = out
        acc[...] = jnp.maximum(acc[...], jnp.maximum(out[:, :LANES], out[:, LANES:]))

    def scores_from_pair(zb, waits=True):
        if waits:
            for k in range(2):
                pair_copy((1 - core) * NZ + zb, k).wait_recv()
        scores((1 - core) * NZ + zb)

    def own_and_pair(step):
        def one(i, carry):
            zb = lax.rem(z + jnp.where(i == 0, NZ - step, step), NZ)
            scores(core * NZ + zb)
            scores_from_pair(zb)
            return carry

        lax.fori_loop(0, 2, one, 0)

    receive(1, 0)
    receive(1, 1)
    prepare()
    scores(own)
    scores_from_pair(z)
    receive(2, 0)
    receive(2, 1)
    own_and_pair(1)
    receive(3, 0)
    receive(3, 1)
    own_and_pair(2)
    receive(4, 0)
    receive(4, 1)
    own_and_pair(3)
    far = lax.rem(z + 4, NZ)
    scores(core * NZ + far)
    scores_from_pair(far)

    def narrow(reduce, r):
        return reduce(acc[r * LANES : (r + 1) * LANES, :].T, axis=0, keepdims=True)

    def spread(row):
        for r in range(ROWS // LANES):
            wide[r * LANES : (r + 1) * LANES, :] = jnp.broadcast_to(row[r : r + 1, :], (LANES, LANES)).T

    def row_copy(phase, k):
        there = on_plane(lax.rem(me + k, NP))
        slot = row_buf.at[phase, me]
        return copy(slot, slot, row_send.at[phase, k], row_recv.at[phase, me], there)

    def across_plane(phase, reduce):
        for r in range(ROWS // LANES):
            row_buf[phase, me, r : r + 1, :] = narrow(reduce, r)

        def send(k, carry):
            row_copy(phase, k).start()
            return carry

        lax.fori_loop(1, NP, send, 0)

        def arrive(k, carry):
            q = lax.rem(me + k, NP)
            slot = row_buf.at[phase, q]
            copy(slot, slot, row_send.at[phase, k], row_recv.at[phase, q], on_plane(q)).wait_recv()
            return carry

        lax.fori_loop(1, NP, arrive, 0)
        return reduce(row_buf[phase], axis=0)

    high = across_plane(0, jnp.max)
    spread(high)

    steps = ROWS // CHUNK

    def by_groups(x):
        return x.reshape(CHUNK // 8, 8, LANES)

    def column_pass(into, term, reduce, start):
        def block(b, carry):
            def some(r, total):
                at = pl.ds(pl.multiple_of(r * CHUNK, CHUNK), CHUNK)
                w = wide[at, :]
                return tuple(
                    reduce[0](total[h], reduce[1](by_groups(term(tile[b, at, h * LANES : (h + 1) * LANES], w)), axis=0))
                    for h in range(2)
                )

            total = lax.fori_loop(0, steps, some, (jnp.full((8, LANES), start, F32),) * 2)
            for h in range(2):
                into[pl.ds(2 * b + h, 1), :] = reduce[1](total[h], axis=0, keepdims=True)
            return carry

        lax.fori_loop(0, BLOCKS, block, 0)

    column_pass(beta, lambda t, w: t - w, (jnp.maximum, jnp.max), -jnp.inf)
    weight[...] = jnp.exp2(beta[...])

    def row_pass(first):
        def rows(r, carry):
            at = pl.ds(pl.multiple_of(r * CHUNK, CHUNK), CHUNK)

            def block(b, total):
                for h in range(2):
                    cut = slice(h * LANES, (h + 1) * LANES)
                    entry = tile[b, at, cut]
                    if first:
                        entry = jnp.exp2(entry - wide[at, :] - beta[pl.ds(2 * b + h, 1), :])
                        tile[b, at, cut] = entry
                    total = total + entry * weight[pl.ds(2 * b + h, 1), :]
                return total

            acc[at, :] = lax.fori_loop(0, BLOCKS, block, jnp.zeros((CHUNK, LANES), F32))
            return carry

        lax.fori_loop(0, steps, rows, 0)

    def halves(step):
        return pl.ds(pl.multiple_of(step * BLOCKS, BLOCKS), BLOCKS)

    def with_pair(phase):
        column_pass(col_stat, lambda t, w: t * w, (jnp.add, jnp.sum), 0.0)
        col_stat[...] = beta[...] + jnp.log2(col_stat[...])
        swap = copy(
            col_stat.at[halves(1 - core), :], pair_buf.at[phase], pair_send.at[phase], pair_recv.at[phase], pair
        )
        swap.start()
        swap.wait()
        return lse2([col_stat[halves(core), :], pair_buf[phase]])

    def round_ring(phase, src, dst):
        def send(k, carry):
            other = lax.rem(z + k, NZ)
            copy(src(other), dst(z), z_send.at[phase, k], z_recv.at[phase, z], on_ring(other)).start()
            return carry

        lax.fori_loop(1, NZ, send, 0)

        def arrive(k, carry):
            other = lax.rem(z + k, NZ)
            copy(src(other), dst(other), z_send.at[phase, k], z_recv.at[phase, other], on_ring(other)).wait_recv()
            return carry

        lax.fori_loop(1, NZ, arrive, 0)

    row_pass(True)
    sums = across_plane(1, jnp.sum)
    spread(jnp.exp2(-log_dst - jnp.log2(sums)))
    z_buf[z] = with_pair(0)
    round_ring(0, lambda other: z_buf.at[z], lambda other: z_buf.at[other])
    delta[halves(core), :] = -log_src - lse2([z_buf[k] for k in range(NZ)])
    half = delta.at[halves(core), :]
    give = copy(half, half, pair_send.at[2], pair_recv.at[2], pair)
    give.start()
    give.wait()
    weight[...] = jnp.exp2(delta[...] + beta[...])

    row_pass(False)
    sums = across_plane(2, jnp.sum)
    spread(jnp.exp2(-log_dst - jnp.log2(sums)))
    for r in range(ROWS // LANES):
        rows = rows_in[r * LANES : (r + 1) * LANES, :]
        row_stat[r : r + 1, :] = jnp.sum((rows * rows).T, axis=0, keepdims=True)
    f_own[...] = row_stat[...] - (log_dst + jnp.log2(sums) + high) / SCALE

    hand = copy(f_own, f_pair, pair_send.at[3], pair_recv.at[3], pair)
    hand.start()
    joined = with_pair(1)
    for k in range(NZ):
        own_buf[k] = joined[2 * k : 2 * k + 2, :]
    fin_buf[z] = own_buf[z]
    round_ring(1, lambda other: own_buf.at[other], lambda other: fin_buf.at[other])
    g_ref[...] = g0_ref[...] - (log_src + lse2([fin_buf[k] for k in range(NZ)])) / SCALE
    hand.wait()
    f_ref[...] = jnp.where(swaps, f_pair[...], f_own[...])

    for step in range(1, 5):
        for k in range(2):
            for way in range(2):
                if step < 4 or k == way:
                    ring_copy(way, step, k, own).wait_send()
    for b in range(NZ):
        for k in range(2):
            pair_copy(core * NZ + b, k).wait_send()
    for phase in range(3):
        def left_row(k, carry):
            row_copy(phase, k).wait_send()
            return carry

        lax.fori_loop(1, NP, left_row, 0)
    for phase in range(2):
        def left_ring(k, carry):
            src = z_buf.at[z] if phase == 0 else own_buf.at[z]
            copy(src, src, z_send.at[phase, k], z_recv.at[phase, z], on_ring(z)).wait_send()
            return carry

        lax.fori_loop(1, NZ, left_ring, 0)


def body(sources, targets, duals_init):
    n_src = sources.shape[0] * lax.axis_size("blk")
    n_dst = targets.shape[0] * lax.axis_size("blk") * lax.axis_size("tgt")
    vmem = pl.BlockSpec(memory_space=pltpu.VMEM)
    dma = pltpu.SemaphoreType.DMA
    f, g = pl.pallas_call(
        functools.partial(kernel, math.log2(n_src), math.log2(n_dst)),
        out_shape=(jax.ShapeDtypeStruct((8, LANES), F32), jax.ShapeDtypeStruct((2, LANES), F32)),
        in_specs=[vmem] * 3,
        out_specs=(vmem, vmem),
        scratch_shapes=[
            pltpu.VMEM((BLOCKS, ROWS, COLS), F32),
            pltpu.VMEM((BLOCKS, HEAD + COLS, D), F32),
            pltpu.VMEM((ROWS, D), F32),
            pltpu.VMEM((ROWS, 4 * D), jnp.bfloat16),
            pltpu.VMEM((ROWS, LANES), F32),
            pltpu.VMEM((ROWS, LANES), F32),
            pltpu.VMEM((8, LANES), F32),
            pltpu.VMEM((2 * BLOCKS, LANES), F32),
            pltpu.VMEM((2 * BLOCKS, LANES), F32),
            pltpu.VMEM((2 * BLOCKS, LANES), F32),
            pltpu.VMEM((2 * BLOCKS, LANES), F32),
            pltpu.VMEM((3, NP, 8, LANES), F32),
            pltpu.VMEM((2, BLOCKS, LANES), F32),
            pltpu.VMEM((NZ, BLOCKS, LANES), F32),
            pltpu.VMEM((NZ, 2, LANES), F32),
            pltpu.VMEM((NZ, 2, LANES), F32),
            pltpu.VMEM((8, LANES), F32),
            pltpu.VMEM((8, LANES), F32),
            dma((2, 7)), dma((2, 7)), dma((16,)), dma((16,)), dma((2,)), dma((2,)),
            dma((3, NP)), dma((3, NP)), dma((2, NZ)), dma((2, NZ)), dma((4,)), dma((4,)),
        ],
        compiler_params=pltpu.CompilerParams(
            collective_id=0, has_side_effects=True, vmem_limit_bytes=60 * 1024 * 1024
        ),
        name="sinkhorn",
    )(sources, targets, duals_init.reshape(2, LANES))
    return f.reshape(-1), g.reshape(-1)


def solution(mesh):
    return jax.shard_map(
        body,
        mesh=mesh,
        in_specs=(P("blk", None), P(("blk", "tgt"), None), P(("blk", "tgt"))),
        out_specs=(P("blk"), P(("blk", "tgt"))),
        check_vma=False,
    )
```

```python
import functools
import math

import jax
import jax.numpy as jnp
from jax import lax
from jax.experimental import pallas as pl
from jax.experimental.pallas import tpu as pltpu
from jax.sharding import PartitionSpec as P

EPS = 0.05
LOG2E = math.log2(math.e)
SCALE = LOG2E / EPS
MESH = pl.DeviceIdType.MESH
NZ = 8
NP = 16
ROWS = 1024
COLS = 256
BLOCKS = 16
HEAD = 8
D = 128
LANES = 128
CHUNK = 128
CUTS = ((0, HEAD + CHUNK), (HEAD + CHUNK, CHUNK))
F32 = jnp.float32


def lse2(parts):
    high = functools.reduce(jnp.maximum, parts)
    total = functools.reduce(jnp.add, [jnp.exp2(p - high) for p in parts])
    return high + jnp.log2(total)


def kernel(
    log_src, log_dst,
    src_ref, tgt_ref, g0_ref, f_ref, g_ref,
    g0, load_sem, tile, kern, blocks, rows_in, lhs, acc, wide,
    top, row_stat, col_stat, gamma, delta, weight,
    row_buf, pair_buf, z_buf, own_buf, fin_buf, f_own, f_pair,
    ring_send, ring_recv, d2d_send, d2d_recv, x_send, x_recv,
    row_send, row_recv, z_send, z_recv, pair_send, pair_recv,
):
    blk, tgt = lax.axis_index("blk"), lax.axis_index("tgt")
    x_lo, z = blk // NZ, lax.rem(blk, NZ)
    core, x_hi, y = lax.rem(tgt, 2), lax.rem(tgt // 2, 2), tgt // 4
    pair = (blk, tgt + 1 - 2 * core)
    me = x_lo * 8 + tgt // 2

    def on_plane(q):
        return (q // 8) * NZ + z, lax.rem(q, 8) * 2 + core

    def on_ring(other):
        return x_lo * NZ + other, tgt

    def beside(step):
        x = lax.rem(2 * x_hi + x_lo + step + 4, 4)
        return lax.rem(x, 2) * NZ + z, y * 4 + (x // 2) * 2 + x_lo

    swaps = core != x_lo
    left, right = beside(-1), beside(1)
    own = core * NZ + z

    loads = [
        pltpu.make_async_copy(tgt_ref, blocks.at[own, pl.ds(HEAD, COLS), :], load_sem.at[0]),
        pltpu.make_async_copy(g0_ref, g0, load_sem.at[1]),
        pltpu.make_async_copy(src_ref, rows_in, load_sem.at[2]),
    ]
    loads[0].start()
    loads[1].start()

    barrier = pltpu.get_barrier_semaphore()
    for k in range(1, NP):
        pl.semaphore_signal(barrier, inc=1, device_id=on_plane(lax.rem(me + k, NP)), device_id_type=MESH)
    for k in range(1, NZ):
        pl.semaphore_signal(barrier, inc=1, device_id=on_ring(lax.rem(z + k, NZ)), device_id_type=MESH)
    pl.semaphore_signal(barrier, inc=1, device_id=pair, device_id_type=MESH)

    @pl.when(swaps)
    def _():
        for there in (left, right):
            pl.semaphore_signal(barrier, inc=1, device_id=there, device_id_type=MESH)

    @pl.when(jnp.logical_not(swaps))
    def _():
        loads[2].start()

    loads[0].wait()
    loads[1].wait()
    for half in range(2):
        part = blocks[own, HEAD + half * LANES : HEAD + (half + 1) * LANES, :]
        norm = jnp.sum((part * part).T, axis=0, keepdims=True)
        blocks[own, half : half + 1, :] = SCALE * (g0[half : half + 1, :] - norm)

    with jax.named_scope("barrier"):
        pl.semaphore_wait(barrier, NP - 1 + NZ - 1 + 1 + 2 * swaps.astype(jnp.int32))

    def copy(src, dst, send, recv, where):
        return pltpu.make_async_remote_copy(
            src_ref=src, dst_ref=dst, send_sem=send, recv_sem=recv, device_id=where, device_id_type=MESH
        )

    def piece(zb, i):
        start, size = CUTS[i % 2]
        return blocks.at[(NZ if i < 2 else 0) + zb, pl.ds(start, size), :]

    def ring_copy(way, step, i, zb):
        to = on_ring(lax.rem(z + (1 if way == 0 else NZ - 1), NZ))
        slot = 4 * (step - 1) + (i if step < 4 else i % 2)
        return copy(piece(zb, i), piece(zb, i), ring_send.at[way, slot], ring_recv.at[way, slot], to)

    def pair_copy(zb, i):
        return copy(piece(zb, i), piece(zb, i), d2d_send.at[4 * zb + i], d2d_recv.at[4 * zb + i], pair)

    def goes(way, step, i):
        return step < 4 or (way == 0) == (i < 2)

    def swap_copy(side):
        at = pl.ds(side * (ROWS // 2), ROWS // 2)
        return copy(src_ref.at[at, :], rows_in.at[at, :], x_send.at[side], x_recv.at[side], (left, right)[side])

    carrier = core == 1

    @pl.when(jnp.logical_not(carrier))
    def _():
        for i in (2, 3):
            pair_copy(z, i).start()

    @pl.when(carrier)
    def _():
        for i in (0, 1):
            for way in range(2):
                ring_copy(way, 1, i, z).start()
            pair_copy(z, i).start()

    @pl.when(swaps)
    def _():
        for side in range(2):
            swap_copy(side).start()

    @pl.when(carrier)
    def _():
        for i in (2, 3):
            pair_copy(z, i).wait_recv()
            for way in range(2):
                ring_copy(way, 1, i, z).start()

    def origin(way, step):
        return lax.rem(z + (NZ - step if way == 0 else step), NZ)

    def receive(step):
        @pl.when(carrier)
        def _():
            for i in range(4):
                for way in range(2):
                    if goes(way, step, i):
                        zb = origin(way, step)
                        ring_copy(way, step, i, zb).wait_recv()
                        if step < 4 and goes(way, step + 1, i):
                            ring_copy(way, step + 1, i, zb).start()
                        pair_copy(zb, i).start()

    def prepare():
        @pl.when(swaps)
        def _():
            for side in range(2):
                swap_copy(side).wait()

        @pl.when(jnp.logical_not(swaps))
        def _():
            loads[2].wait()

        for r in range(ROWS // LANES):
            rows = rows_in[r * LANES : (r + 1) * LANES, :] * (2 * SCALE)
            high = rows.astype(jnp.bfloat16)
            low = (rows - high.astype(F32)).astype(jnp.bfloat16)
            lhs[r * LANES : (r + 1) * LANES, :] = jnp.concatenate([high, low, high, low], axis=1)
        top[...] = jnp.full_like(top, -jnp.inf)
        acc[...] = jnp.zeros_like(acc)

    def scores(zb):
        outs, heads, at = [], [], []
        for which in (core, 1 - core):
            b = which * NZ + zb
            t = blocks[b, HEAD:, :]
            high = t.astype(jnp.bfloat16)
            low = (t - high.astype(F32)).astype(jnp.bfloat16)
            rhs = jnp.concatenate([high, high, low, low], axis=1)
            outs.append(lax.dot_general(lhs[...], rhs, (((1,), (1,)), ((), ())), preferred_element_type=F32))
            heads += [jnp.broadcast_to(blocks[b, h : h + 1, :], (8, LANES)) for h in range(2)]
            at.append(b)
        for k in range(0, ROWS, 8):
            rows = slice(k, k + 8)
            parts = []
            for c in range(4):
                cut = slice((c % 2) * LANES, (c % 2 + 1) * LANES)
                parts.append(outs[c // 2][rows, cut] + heads[c])
                tile[at[c // 2], rows, cut] = parts[c]
            old = top[rows, :]
            new = jnp.maximum(jnp.maximum(parts[0], parts[1]), jnp.maximum(parts[2], parts[3]))
            new = jnp.maximum(old, new)
            top[rows, :] = new
            e = [jnp.exp2(p - new) for p in parts]
            acc[rows, :] = acc[rows, :] * jnp.exp2(old - new) + ((e[0] + e[1]) + (e[2] + e[3]))

    def scores_at(zb):
        @pl.when(jnp.logical_not(carrier))
        def _():
            for i in range(4):
                pair_copy(zb, i).wait_recv()

        scores(zb)

    def scores_beside(step):
        def one(i, carry):
            scores_at(lax.rem(z + jnp.where(i == 0, NZ - step, step), NZ))
            return carry

        lax.fori_loop(0, 2, one, 0)

    with jax.named_scope("receive_1"):
        receive(1)
    with jax.named_scope("prepare"):
        prepare()
    with jax.named_scope("scores_0"):
        @pl.when(jnp.logical_not(carrier))
        def _():
            for i in range(2):
                pair_copy(z, i).wait_recv()

        scores(z)
    with jax.named_scope("receive_2"):
        receive(2)
    with jax.named_scope("scores_1"):
        scores_beside(1)
    with jax.named_scope("receive_3"):
        receive(3)
    with jax.named_scope("scores_2"):
        scores_beside(2)
    with jax.named_scope("receive_4"):
        receive(4)
    with jax.named_scope("scores_3"):
        scores_beside(3)
    with jax.named_scope("scores_4"):
        scores_at(lax.rem(z + 4, NZ))

    def spread(row):
        for r in range(ROWS // LANES):
            wide[r * LANES : (r + 1) * LANES, :] = jnp.broadcast_to(row[r : r + 1, :], (LANES, LANES)).T

    def across_plane(phase):
        def send(k, carry):
            q = lax.rem(me + k, NP)
            slot = row_buf.at[phase, me]
            copy(slot, slot, row_send.at[phase, k], row_recv.at[phase, me], on_plane(q)).start()
            return carry

        lax.fori_loop(1, NP, send, 0)

        def arrive(k, carry):
            q = lax.rem(me + k, NP)
            slot = row_buf.at[phase, q]
            copy(slot, slot, row_send.at[phase, k], row_recv.at[phase, q], on_plane(q)).wait_recv()
            return carry

        lax.fori_loop(1, NP, arrive, 0)

    def tree(op, xs):
        while len(xs) > 1:
            xs = [op(*xs[i : i + 2]) if i + 1 < len(xs) else xs[i] for i in range(0, len(xs), 2)]
        return xs[0]

    QUAD = 4
    TALL = 256

    def quads(core_of):
        return [core_of * NZ + q * QUAD for q in range(NZ // QUAD)]

    def pick(x, k, h):
        return x[8 * k : 8 * k + 8, h * LANES : (h + 1) * LANES]

    def summed(op, xs):
        return op(functools.reduce(op, xs[0::2]), functools.reduce(op, xs[1::2])) if len(xs) > 1 else xs[0]

    def column_pass(first, into, held, term, op, start):
        def some(r, total):
            at = pl.ds(pl.multiple_of(r * TALL, TALL), TALL)
            w = wide.at[at, :]
            result = []
            for q in range(QUAD):
                view = held.at[first + q, at, :]
                for h in range(2):
                    xs = [term(pick(view, k, h), w[8 * k : 8 * k + 8, :]) for k in range(TALL // 8)]
                    result.append(op(total[2 * q + h], summed(op, xs)))
            return tuple(result)

        total = lax.fori_loop(0, ROWS // TALL, some, (jnp.full((8, LANES), start, F32),) * (2 * QUAD))
        fold = jnp.max if op is jnp.maximum else jnp.sum
        for c in range(2 * QUAD):
            into[pl.ds(2 * first + c, 1), :] = fold(total[c], axis=0, keepdims=True)

    def exp_pass(first):
        tall = 128

        def some(r, total):
            at = pl.ds(pl.multiple_of(r * tall, tall), tall)
            w = wide[at, :]
            result = []
            for q in range(QUAD):
                view = tile.at[first + q, at, :]
                out = kern.at[first + q, at, :]
                for h in range(2):
                    low = gamma[pl.ds(2 * (first + q) + h, 1), :]
                    entry = jnp.exp2((view[:, h * LANES : (h + 1) * LANES] + w) - low)
                    out[:, h * LANES : (h + 1) * LANES] = entry
                    result.append(total[2 * q + h] + jnp.sum(entry.reshape(tall // 8, 8, LANES), axis=0))
            return tuple(result)

        total = lax.fori_loop(0, ROWS // tall, some, (jnp.zeros((8, LANES), F32),) * (2 * QUAD))
        for c in range(2 * QUAD):
            col_stat[pl.ds(2 * first + c, 1), :] = jnp.sum(total[c], axis=0, keepdims=True)

    def row_pass(first, fresh):
        v = [weight[pl.ds(2 * first + c, 1), :] for c in range(2 * QUAD)]

        def some(r, carry):
            at = pl.ds(pl.multiple_of(r * TALL, TALL), TALL)
            views = [kern.at[first + q, at, :] for q in range(QUAD)]
            out = acc.at[at, :]
            for k in range(TALL // 8):
                total = summed(jnp.add, [pick(views[c // 2], k, c % 2) * v[c] for c in range(2 * QUAD)])
                out[8 * k : 8 * k + 8, :] = total if fresh else out[8 * k : 8 * k + 8, :] + total
            return carry

        lax.fori_loop(0, ROWS // TALL, some, 0)

    def halves(step):
        return pl.ds(pl.multiple_of(step * BLOCKS, BLOCKS), BLOCKS)

    def log_sums(core_of):
        rows = halves(core_of)
        col_stat[rows, :] = gamma[rows, :] + jnp.log2(col_stat[rows, :])

    def with_pair(phase, columns):
        for first in quads(1 - core):
            columns(first)
        log_sums(1 - core)
        rows = halves(1 - core)
        swap = copy(col_stat.at[rows, :], pair_buf.at[phase], pair_send.at[phase], pair_recv.at[phase], pair)
        swap.start()
        for first in quads(core):
            columns(first)
        log_sums(core)
        swap.wait()
        return lse2([col_stat[halves(core), :], pair_buf[phase]])

    def round_ring(phase, src, dst):
        def send(k, carry):
            other = lax.rem(z + k, NZ)
            copy(src(other), dst(z), z_send.at[phase, k], z_recv.at[phase, z], on_ring(other)).start()
            return carry

        lax.fori_loop(1, NZ, send, 0)

        def arrive(k, carry):
            other = lax.rem(z + k, NZ)
            copy(src(other), dst(other), z_send.at[phase, k], z_recv.at[phase, other], on_ring(other)).wait_recv()
            return carry

        lax.fori_loop(1, NZ, arrive, 0)

    with jax.named_scope("row_lse"):
        for r in range(ROWS // LANES):
            at = slice(r * LANES, (r + 1) * LANES)
            lane_top = top[at, :].T
            high = jnp.max(lane_top, axis=0, keepdims=True)
            total = jnp.sum(acc[at, :].T * jnp.exp2(lane_top - high), axis=0, keepdims=True)
            row_buf[0, me, r : r + 1, :] = high + jnp.log2(total)
    with jax.named_scope("plane_0"):
        across_plane(0)
    with jax.named_scope("spread"):
        phi = -log_dst - lse2([row_buf[0, q] for q in range(NP)])
        spread(phi)
    with jax.named_scope("gamma"):
        for which in range(2):
            for first in quads(which):
                column_pass(first, gamma, tile, jnp.add, jnp.maximum, -jnp.inf)
    with jax.named_scope("exp"):
        z_buf[z] = with_pair(0, exp_pass)
    with jax.named_scope("ring_0"):
        round_ring(0, lambda other: z_buf.at[z], lambda other: z_buf.at[other])
    delta[halves(core), :] = -log_src - lse2([z_buf[k] for k in range(NZ)])
    half = delta.at[halves(core), :]
    give = copy(half, half, pair_send.at[2], pair_recv.at[2], pair)
    give.start()

    def weigh(core_of):
        rows = halves(core_of)
        weight[rows, :] = jnp.exp2(delta[rows, :] + gamma[rows, :])

    with jax.named_scope("rows_own"):
        weigh(core)
        for n, first in enumerate(quads(core)):
            row_pass(first, n == 0)
    with jax.named_scope("give"):
        give.wait()
    with jax.named_scope("rows_pair"):
        weigh(1 - core)
        for first in quads(1 - core):
            row_pass(first, False)
        for r in range(ROWS // LANES):
            at = slice(r * LANES, (r + 1) * LANES)
            row_buf[1, me, r : r + 1, :] = jnp.sum(acc[at, :].T, axis=0, keepdims=True)
    with jax.named_scope("plane_1"):
        across_plane(1)
    with jax.named_scope("spread"):
        log_sum = log_dst + jnp.log2(jnp.sum(row_buf[1], axis=0))
        spread(jnp.exp2(-log_sum))
    with jax.named_scope("f"):
        for r in range(ROWS // LANES):
            rows = rows_in[r * LANES : (r + 1) * LANES, :]
            row_stat[r : r + 1, :] = jnp.sum((rows * rows).T, axis=0, keepdims=True)
        f_own[...] = row_stat[...] + (phi - log_sum) / SCALE

    hand = copy(f_own, f_pair, pair_send.at[3], pair_recv.at[3], pair)
    hand.start()
    with jax.named_scope("cols"):
        joined = with_pair(1, lambda first: column_pass(first, col_stat, kern, jnp.multiply, jnp.add, 0.0))
    for k in range(NZ):
        own_buf[k] = joined[2 * k : 2 * k + 2, :]
    fin_buf[z] = own_buf[z]
    with jax.named_scope("ring_1"):
        round_ring(1, lambda other: own_buf.at[other], lambda other: fin_buf.at[other])
    g_ref[...] = g0[...] - (log_src + lse2([fin_buf[k] for k in range(NZ)])) / SCALE
    hand.wait()
    f_ref[...] = jnp.where(swaps, f_pair[...], f_own[...])

    @pl.when(carrier)
    def _():
        for step in range(1, 5):
            for i in range(4):
                for way in range(2):
                    if goes(way, step, i):
                        ring_copy(way, step, i, z).wait_send()
        for i in range(2):
            pair_copy(z, i).wait_send()
        for step in range(1, 5):
            for way in range(2):
                for i in range(4):
                    if goes(way, step, i):
                        pair_copy(origin(way, step), i).wait_send()

    @pl.when(jnp.logical_not(carrier))
    def _():
        for i in (2, 3):
            pair_copy(z, i).wait_send()

    for phase in range(2):
        def left_row(k, carry):
            slot = row_buf.at[phase, me]
            copy(slot, slot, row_send.at[phase, k], row_recv.at[phase, me], pair).wait_send()
            return carry

        lax.fori_loop(1, NP, left_row, 0)
    for phase in range(2):
        def left_ring(k, carry):
            src = z_buf.at[z] if phase == 0 else own_buf.at[z]
            copy(src, src, z_send.at[phase, k], z_recv.at[phase, z], on_ring(z)).wait_send()
            return carry

        lax.fori_loop(1, NZ, left_ring, 0)


def body(sources, targets, duals_init):
    n_src = sources.shape[0] * lax.axis_size("blk")
    n_dst = targets.shape[0] * lax.axis_size("blk") * lax.axis_size("tgt")
    vmem = pl.BlockSpec(memory_space=pltpu.VMEM)
    dma = pltpu.SemaphoreType.DMA
    f, g = pl.pallas_call(
        functools.partial(kernel, math.log2(n_src), math.log2(n_dst)),
        out_shape=(jax.ShapeDtypeStruct((8, LANES), F32), jax.ShapeDtypeStruct((2, LANES), F32)),
        in_specs=[pl.BlockSpec(memory_space=pl.ANY)] * 3,
        out_specs=(vmem, vmem),
        scratch_shapes=[
            pltpu.VMEM((2, LANES), F32),
            dma((3,)),
            pltpu.VMEM((BLOCKS, ROWS, COLS), F32),
            pltpu.VMEM((BLOCKS, ROWS, COLS), F32),
            pltpu.VMEM((BLOCKS, HEAD + COLS, D), F32),
            pltpu.VMEM((ROWS, D), F32),
            pltpu.VMEM((ROWS, 4 * D), jnp.bfloat16),
            pltpu.VMEM((ROWS, LANES), F32),
            pltpu.VMEM((ROWS, LANES), F32),
            pltpu.VMEM((ROWS, LANES), F32),
            pltpu.VMEM((8, LANES), F32),
            pltpu.VMEM((2 * BLOCKS, LANES), F32),
            pltpu.VMEM((2 * BLOCKS, LANES), F32),
            pltpu.VMEM((2 * BLOCKS, LANES), F32),
            pltpu.VMEM((2 * BLOCKS, LANES), F32),
            pltpu.VMEM((2, NP, 8, LANES), F32),
            pltpu.VMEM((2, BLOCKS, LANES), F32),
            pltpu.VMEM((NZ, BLOCKS, LANES), F32),
            pltpu.VMEM((NZ, 2, LANES), F32),
            pltpu.VMEM((NZ, 2, LANES), F32),
            pltpu.VMEM((8, LANES), F32),
            pltpu.VMEM((8, LANES), F32),
            dma((2, 14)), dma((2, 14)), dma((32,)), dma((32,)), dma((2,)), dma((2,)),
            dma((2, NP)), dma((2, NP)), dma((2, NZ)), dma((2, NZ)), dma((4,)), dma((4,)),
        ],
        compiler_params=pltpu.CompilerParams(
            collective_id=0, has_side_effects=True, vmem_limit_bytes=60 * 1024 * 1024
        ),
        name="sinkhorn",
    )(sources, targets, duals_init.reshape(2, LANES))
    return f.reshape(-1), g.reshape(-1)


def solution(mesh):
    return jax.shard_map(
        body,
        mesh=mesh,
        in_specs=(P("blk", None), P(("blk", "tgt"), None), P(("blk", "tgt"))),
        out_specs=(P("blk"), P(("blk", "tgt"))),
        check_vma=False,
    )
```

```python
import functools
import math

import jax
import jax.numpy as jnp
from jax import lax
from jax.experimental import pallas as pl
from jax.experimental.pallas import tpu as pltpu
from jax.sharding import PartitionSpec as P

EPS = 0.05
LOG2E = math.log2(math.e)
SCALE = LOG2E / EPS
MESH = pl.DeviceIdType.MESH
NZ = 8
NP = 16
ROWS = 1024
COLS = 256
BLOCKS = 16
HEAD = 8
D = 128
LANES = 128
CHUNK = 128
CUTS = ((0, HEAD + CHUNK), (HEAD + CHUNK, CHUNK))
F32 = jnp.float32


def lse2(parts):
    high = functools.reduce(jnp.maximum, parts)
    total = functools.reduce(jnp.add, [jnp.exp2(p - high) for p in parts])
    return high + jnp.log2(total)


def kernel(
    log_src, log_dst,
    src_ref, tgt_ref, g0_ref, f_ref, g_ref,
    g0, load_sem, tile, kern, blocks, rows_in, lhs, acc, wide,
    top, row_stat, col_stat, gamma, delta, weight,
    row_buf, pair_buf, z_buf, own_buf, fin_buf, f_own, f_pair,
    ring_send, ring_recv, d2d_send, d2d_recv, x_send, x_recv,
    row_send, row_recv, z_send, z_recv, pair_send, pair_recv,
):
    blk, tgt = lax.axis_index("blk"), lax.axis_index("tgt")
    x_lo, z = blk // NZ, lax.rem(blk, NZ)
    core, x_hi, y = lax.rem(tgt, 2), lax.rem(tgt // 2, 2), tgt // 4
    pair = (blk, tgt + 1 - 2 * core)
    me = x_lo * 8 + tgt // 2

    def on_plane(q):
        return (q // 8) * NZ + z, lax.rem(q, 8) * 2 + core

    def on_ring(other):
        return x_lo * NZ + other, tgt

    def beside(step):
        x = lax.rem(2 * x_hi + x_lo + step + 4, 4)
        return lax.rem(x, 2) * NZ + z, y * 4 + (x // 2) * 2 + x_lo

    swaps = core != x_lo
    left, right = beside(-1), beside(1)
    own = core * NZ + z

    loads = [
        pltpu.make_async_copy(tgt_ref, blocks.at[own, pl.ds(HEAD, COLS), :], load_sem.at[0]),
        pltpu.make_async_copy(g0_ref, g0, load_sem.at[1]),
        pltpu.make_async_copy(src_ref, rows_in, load_sem.at[2]),
    ]
    loads[0].start()
    loads[1].start()

    barrier = pltpu.get_barrier_semaphore()
    for k in range(1, NP):
        pl.semaphore_signal(barrier, inc=1, device_id=on_plane(lax.rem(me + k, NP)), device_id_type=MESH)
    for k in range(1, NZ):
        pl.semaphore_signal(barrier, inc=1, device_id=on_ring(lax.rem(z + k, NZ)), device_id_type=MESH)
    pl.semaphore_signal(barrier, inc=1, device_id=pair, device_id_type=MESH)

    @pl.when(swaps)
    def _():
        for there in (left, right):
            pl.semaphore_signal(barrier, inc=1, device_id=there, device_id_type=MESH)

    @pl.when(jnp.logical_not(swaps))
    def _():
        loads[2].start()

    loads[0].wait()
    loads[1].wait()
    for half in range(2):
        part = blocks[own, HEAD + half * LANES : HEAD + (half + 1) * LANES, :]
        norm = jnp.sum((part * part).T, axis=0, keepdims=True)
        blocks[own, half : half + 1, :] = SCALE * (g0[half : half + 1, :] - norm)

    with jax.named_scope("barrier"):
        pl.semaphore_wait(barrier, NP - 1 + NZ - 1 + 1 + 2 * swaps.astype(jnp.int32))

    def copy(src, dst, send, recv, where):
        return pltpu.make_async_remote_copy(
            src_ref=src, dst_ref=dst, send_sem=send, recv_sem=recv, device_id=where, device_id_type=MESH
        )

    def piece(zb, i):
        start, size = CUTS[i % 2]
        return blocks.at[(NZ if i < 2 else 0) + zb, pl.ds(start, size), :]

    def ring_copy(way, step, i, zb):
        to = on_ring(lax.rem(z + (1 if way == 0 else NZ - 1), NZ))
        slot = 4 * (step - 1) + (i if step < 4 else i % 2)
        return copy(piece(zb, i), piece(zb, i), ring_send.at[way, slot], ring_recv.at[way, slot], to)

    def pair_copy(zb, i):
        return copy(piece(zb, i), piece(zb, i), d2d_send.at[4 * zb + i], d2d_recv.at[4 * zb + i], pair)

    def goes(way, step, i):
        return step < 4 or (way == 0) == (i < 2)

    def swap_copy(side):
        at = pl.ds(side * (ROWS // 2), ROWS // 2)
        return copy(src_ref.at[at, :], rows_in.at[at, :], x_send.at[side], x_recv.at[side], (left, right)[side])

    carrier = core == 1

    @pl.when(jnp.logical_not(carrier))
    def _():
        for i in (2, 3):
            pair_copy(z, i).start()

    @pl.when(carrier)
    def _():
        for i in (0, 1):
            for way in range(2):
                ring_copy(way, 1, i, z).start()
            pair_copy(z, i).start()

    @pl.when(swaps)
    def _():
        for side in range(2):
            swap_copy(side).start()

    @pl.when(carrier)
    def _():
        for i in (2, 3):
            pair_copy(z, i).wait_recv()
            for way in range(2):
                ring_copy(way, 1, i, z).start()

    def origin(way, step):
        return lax.rem(z + (NZ - step if way == 0 else step), NZ)

    def receive(step, half):
        @pl.when(carrier)
        def _():
            for i in range(2):
                start, size = CUTS[i]
                for way in range(2):
                    zb = origin(way, step)
                    part = blocks.at[(1 - half) * NZ + zb, pl.ds(start, size), :]
                    to = on_ring(lax.rem(z + (1 if way == 0 else NZ - 1), NZ))
                    slot = 4 * (step - 1) + 2 * half + i
                    came = copy(part, part, ring_send.at[way, slot], ring_recv.at[way, slot], to)
                    came.wait_recv()
                    last = step == 3
                    far = 12 + i
                    slot = jnp.where(last, far, slot + 4)

                    @pl.when(jnp.logical_or(jnp.logical_not(last), (half == 0) == (way == 0)))
                    def _():
                        copy(part, part, ring_send.at[way, slot], ring_recv.at[way, slot], to).start()

                    at = 4 * zb + 2 * half + i
                    copy(part, part, d2d_send.at[at], d2d_recv.at[at], pair).start()

    def receive_far():
        @pl.when(carrier)
        def _():
            for i in range(4):
                way = 0 if i < 2 else 1
                zb = origin(way, 4)
                ring_copy(way, 4, i, zb).wait_recv()
                pair_copy(zb, i).start()

    def prepare():
        @pl.when(swaps)
        def _():
            for side in range(2):
                swap_copy(side).wait()

        @pl.when(jnp.logical_not(swaps))
        def _():
            loads[2].wait()

        for r in range(ROWS // LANES):
            rows = rows_in[r * LANES : (r + 1) * LANES, :] * (2 * SCALE)
            high = rows.astype(jnp.bfloat16)
            low = (rows - high.astype(F32)).astype(jnp.bfloat16)
            lhs[r * LANES : (r + 1) * LANES, :] = jnp.concatenate([high, low, high, low], axis=1)
        top[...] = jnp.full_like(top, -jnp.inf)
        acc[...] = jnp.zeros_like(acc)

    def scores(zb):
        outs, heads, at = [], [], []
        for which in (core, 1 - core):
            b = which * NZ + zb
            t = blocks[b, HEAD:, :]
            high = t.astype(jnp.bfloat16)
            low = (t - high.astype(F32)).astype(jnp.bfloat16)
            rhs = jnp.concatenate([high, high, low, low], axis=1)
            outs.append(lax.dot_general(lhs[...], rhs, (((1,), (1,)), ((), ())), preferred_element_type=F32))
            heads += [jnp.broadcast_to(blocks[b, h : h + 1, :], (8, LANES)) for h in range(2)]
            at.append(b)
        for k in range(0, ROWS, 8):
            rows = slice(k, k + 8)
            parts = []
            for c in range(4):
                cut = slice((c % 2) * LANES, (c % 2 + 1) * LANES)
                parts.append(outs[c // 2][rows, cut] + heads[c])
                tile[at[c // 2], rows, cut] = parts[c]
            old = top[rows, :]
            new = jnp.maximum(jnp.maximum(parts[0], parts[1]), jnp.maximum(parts[2], parts[3]))
            new = jnp.maximum(old, new)
            top[rows, :] = new
            e = [jnp.exp2(p - new) for p in parts]
            acc[rows, :] = acc[rows, :] * jnp.exp2(old - new) + ((e[0] + e[1]) + (e[2] + e[3]))

    def scores_step(n, carry):
        step = n // 2 + 1
        half = lax.rem(n, 2)

        @pl.when(jnp.logical_and(n >= 2, n < 6))
        def _():
            receive(step, half)

        @pl.when(n == 2 * NZ // 2)
        def _():
            receive_far()

        off = n // 2
        zb = lax.rem(z + jnp.where(half == 0, NZ - off, off), NZ)

        @pl.when(jnp.logical_not(carrier))
        def _():
            for i in range(2):
                pair_copy(zb, i).wait_recv()

            @pl.when(n > 1)
            def _():
                for i in (2, 3):
                    pair_copy(zb, i).wait_recv()

        scores(zb)
        return carry

    with jax.named_scope("receive_1"):
        receive(1, 0)
        receive(1, 1)
    with jax.named_scope("prepare"):
        prepare()
    with jax.named_scope("scores"):
        lax.fori_loop(1, NZ + 1, scores_step, 0)

    def spread(row):
        for r in range(ROWS // LANES):
            wide[r * LANES : (r + 1) * LANES, :] = jnp.broadcast_to(row[r : r + 1, :], (LANES, LANES)).T

    x_at = 2 * x_hi + x_lo

    def off_plane(dx, dy):
        x, row = lax.rem(x_at + dx, 4), lax.rem(y + dy, 4)
        return lax.rem(x, 2) * NZ + z, row * 4 + (x // 2) * 2 + core

    def plane_copies(phase):
        slot = row_buf.at[phase, me]
        ways = sorted(
            ((dx, dy) for dx in range(4) for dy in range(4) if dx or dy),
            key=lambda d: -min(d[0], 4 - d[0]) - min(d[1], 4 - d[1]),
        )
        return [
            copy(slot, slot, row_send.at[phase, k], row_recv.at[phase, me], off_plane(*d)) for k, d in enumerate(ways)
        ]

    def across_plane(phase, meanwhile):
        for c in plane_copies(phase):
            c.start()
        meanwhile()

        def arrive(k, carry):
            q = lax.rem(me + k, NP)
            slot = row_buf.at[phase, q]
            copy(slot, slot, row_send.at[phase, 0], row_recv.at[phase, q], pair).wait_recv()
            return carry

        lax.fori_loop(1, NP, arrive, 0)

    def plane_sent(phase):
        for c in plane_copies(phase):
            c.wait_send()

    QUAD = 4
    TALL = 256

    def quads(core_of):
        return [core_of * NZ + q * QUAD for q in range(NZ // QUAD)]

    def pick(x, k, h):
        return x[8 * k : 8 * k + 8, h * LANES : (h + 1) * LANES]

    def summed(op, xs):
        return op(functools.reduce(op, xs[0::2]), functools.reduce(op, xs[1::2])) if len(xs) > 1 else xs[0]

    def column_pass(first, into, held, term, op, start):
        def some(r, total):
            at = pl.ds(pl.multiple_of(r * TALL, TALL), TALL)
            w = wide.at[at, :]
            result = []
            for q in range(QUAD):
                view = held.at[first + q, at, :]
                for h in range(2):
                    xs = [term(pick(view, k, h), w[8 * k : 8 * k + 8, :]) for k in range(TALL // 8)]
                    result.append(op(total[2 * q + h], summed(op, xs)))
            return tuple(result)

        total = lax.fori_loop(0, ROWS // TALL, some, (jnp.full((8, LANES), start, F32),) * (2 * QUAD))
        fold = jnp.max if op is jnp.maximum else jnp.sum
        for c in range(2 * QUAD):
            into[pl.ds(2 * first + c, 1), :] = fold(total[c], axis=0, keepdims=True)

    def exp_pass(first):
        tall = 256

        def some(r, total):
            at = pl.ds(pl.multiple_of(r * tall, tall), tall)
            w = wide[at, :]
            result = []
            for q in range(QUAD):
                view = tile.at[first + q, at, :]
                out = kern.at[first + q, at, :]
                for h in range(2):
                    low = gamma[pl.ds(2 * (first + q) + h, 1), :]
                    entry = jnp.exp2((view[:, h * LANES : (h + 1) * LANES] + w) - low)
                    out[:, h * LANES : (h + 1) * LANES] = entry
                    result.append(total[2 * q + h] + jnp.sum(entry.reshape(tall // 8, 8, LANES), axis=0))
            return tuple(result)

        total = lax.fori_loop(0, ROWS // tall, some, (jnp.zeros((8, LANES), F32),) * (2 * QUAD))
        for c in range(2 * QUAD):
            col_stat[pl.ds(2 * first + c, 1), :] = jnp.sum(total[c], axis=0, keepdims=True)

    def row_pass(first, fresh):
        v = [weight[pl.ds(2 * first + c, 1), :] for c in range(2 * QUAD)]

        def some(r, carry):
            at = pl.ds(pl.multiple_of(r * TALL, TALL), TALL)
            views = [kern.at[first + q, at, :] for q in range(QUAD)]
            out = acc.at[at, :]
            for k in range(TALL // 8):
                total = summed(jnp.add, [pick(views[c // 2], k, c % 2) * v[c] for c in range(2 * QUAD)])
                out[8 * k : 8 * k + 8, :] = total if fresh else out[8 * k : 8 * k + 8, :] + total
            return carry

        lax.fori_loop(0, ROWS // TALL, some, 0)

    def halves(step):
        return pl.ds(pl.multiple_of(step * BLOCKS, BLOCKS), BLOCKS)

    def quad_rows(first):
        return pl.ds(pl.multiple_of(2 * first, 8), 8)

    def with_pair(phase, columns, emit):
        swaps_out = []
        for q, first in enumerate(quads(1 - core)):
            columns(first)
            rows = quad_rows(first)
            col_stat[rows, :] = gamma[rows, :] + jnp.log2(col_stat[rows, :])
            to = pair_buf.at[phase, pl.ds(8 * q, 8), :]
            k = 2 * phase + q
            swaps_out.append(copy(col_stat.at[rows, :], to, pair_send.at[k], pair_recv.at[k], pair))
            swaps_out[q].start()
        for q, first in enumerate(quads(core)):
            columns(first)
            rows = quad_rows(first)
            part = gamma[rows, :] + jnp.log2(col_stat[rows, :])
            swaps_out[q].wait()
            emit(q, lse2([part, pair_buf[phase, 8 * q : 8 * q + 8, :]]))

    def ring_copies(q):
        part = z_buf.at[z, pl.ds(8 * q, 8), :]
        return [
            copy(part, part, z_send.at[q, k], z_recv.at[q, z], on_ring(lax.rem(z + k, NZ))) for k in (4, 3, 5, 2, 6, 1, 7)
        ]

    def ring_waits(slots):
        def arrive(k, carry):
            other = lax.rem(z + k, NZ)
            for phase, ref in slots:
                part = ref(other)
                copy(part, part, z_send.at[phase, 0], z_recv.at[phase, other], pair).wait_recv()
            return carry

        lax.fori_loop(1, NZ, arrive, 0)

    with jax.named_scope("row_lse"):
        for r in range(ROWS // LANES):
            at = slice(r * LANES, (r + 1) * LANES)
            lane_top = top[at, :].T
            high = jnp.max(lane_top, axis=0, keepdims=True)
            total = jnp.sum(acc[at, :].T * jnp.exp2(lane_top - high), axis=0, keepdims=True)
            row_buf[0, me, r : r + 1, :] = high + jnp.log2(total)

    def after_gather():
        for r in range(ROWS // LANES):
            rows = rows_in[r * LANES : (r + 1) * LANES, :]
            row_stat[r : r + 1, :] = jnp.sum((rows * rows).T, axis=0, keepdims=True)

        @pl.when(carrier)
        def _():
            for step in range(1, 5):
                for i in range(4):
                    for way in range(2):
                        if goes(way, step, i):
                            ring_copy(way, step, i, z).wait_send()
                            pair_copy(origin(way, step), i).wait_send()
            for i in range(2):
                pair_copy(z, i).wait_send()

        @pl.when(jnp.logical_not(carrier))
        def _():
            for i in (2, 3):
                pair_copy(z, i).wait_send()

    with jax.named_scope("plane_0"):
        across_plane(0, after_gather)
    with jax.named_scope("spread"):
        phi = -log_dst - lse2([row_buf[0, q] for q in range(NP)])
        spread(phi)

    def first_columns(first):
        column_pass(first, gamma, tile, jnp.add, jnp.maximum, -jnp.inf)
        exp_pass(first)

    def to_ring(q, joined):
        z_buf[z, 8 * q : 8 * q + 8, :] = joined
        for c in ring_copies(q):
            c.start()

    with jax.named_scope("exp"):
        with_pair(0, first_columns, to_ring)
    with jax.named_scope("ring_0"):
        ring_waits([(q, lambda other, q=q: z_buf.at[other, pl.ds(8 * q, 8), :]) for q in range(2)])
    delta[halves(core), :] = -log_src - lse2([z_buf[k] for k in range(NZ)])
    half = delta.at[halves(core), :]
    give = copy(half, half, pair_send.at[4], pair_recv.at[4], pair)
    give.start()

    def weigh(core_of):
        rows = halves(core_of)
        weight[rows, :] = jnp.exp2(delta[rows, :] + gamma[rows, :])

    with jax.named_scope("rows_own"):
        weigh(core)
        for n, first in enumerate(quads(core)):
            row_pass(first, n == 0)
    with jax.named_scope("give"):
        give.wait()
    with jax.named_scope("rows_pair"):
        weigh(1 - core)
        for first in quads(1 - core):
            row_pass(first, False)
        for r in range(ROWS // LANES):
            at = slice(r * LANES, (r + 1) * LANES)
            row_buf[1, me, r : r + 1, :] = jnp.sum(acc[at, :].T, axis=0, keepdims=True)

    def after_ring():
        plane_sent(0)
        for q in range(2):
            for c in ring_copies(q):
                c.wait_send()

    with jax.named_scope("plane_1"):
        across_plane(1, after_ring)
    with jax.named_scope("spread"):
        log_sum = log_dst + jnp.log2(jnp.sum(row_buf[1], axis=0))
        spread(jnp.exp2(-log_sum))
        f_own[...] = row_stat[...] + (phi - log_sum) / SCALE
    hand = copy(f_own, f_pair, pair_send.at[5], pair_recv.at[5], pair)
    hand.start()

    def part_copy(to):
        return copy(own_buf.at[to], fin_buf.at[z], z_send.at[2, to], z_recv.at[2, z], on_ring(to))

    def to_owners(q, joined):
        for i in range(NZ // 2):
            to = NZ // 2 * q + i
            part = joined[2 * i : 2 * i + 2, :]
            own_buf[to] = part

            @pl.when(z == to)
            def _():
                fin_buf[to] = part

            @pl.when(z != to)
            def _():
                part_copy(to).start()

    with jax.named_scope("cols"):
        with_pair(1, lambda first: column_pass(first, col_stat, kern, jnp.multiply, jnp.add, 0.0), to_owners)
    with jax.named_scope("ring_1"):
        plane_sent(1)
        hand.wait()
        f_ref[...] = jnp.where(swaps, f_pair[...], f_own[...])
        ring_waits([(2, lambda other: fin_buf.at[other])])
    g_ref[...] = g0[...] - (log_src + lse2([fin_buf[k] for k in range(NZ)])) / SCALE
    for to in range(NZ):

        @pl.when(z != to)
        def _():
            part_copy(to).wait_send()


def body(sources, targets, duals_init):
    n_src = sources.shape[0] * lax.axis_size("blk")
    n_dst = targets.shape[0] * lax.axis_size("blk") * lax.axis_size("tgt")
    vmem = pl.BlockSpec(memory_space=pltpu.VMEM)
    dma = pltpu.SemaphoreType.DMA
    f, g = pl.pallas_call(
        functools.partial(kernel, math.log2(n_src), math.log2(n_dst)),
        out_shape=(pltpu.VMEM((8, LANES), F32), pltpu.VMEM((2, LANES), F32)),
        in_specs=[pl.BlockSpec(memory_space=pl.ANY)] * 3,
        out_specs=(vmem, vmem),
        scratch_shapes=[
            pltpu.VMEM((2, LANES), F32),
            dma((3,)),
            pltpu.VMEM((BLOCKS, ROWS, COLS), F32),
            pltpu.VMEM((BLOCKS, ROWS, COLS), F32),
            pltpu.VMEM((BLOCKS, HEAD + COLS, D), F32),
            pltpu.VMEM((ROWS, D), F32),
            pltpu.VMEM((ROWS, 4 * D), jnp.bfloat16),
            pltpu.VMEM((ROWS, LANES), F32),
            pltpu.VMEM((ROWS, LANES), F32),
            pltpu.VMEM((ROWS, LANES), F32),
            pltpu.VMEM((8, LANES), F32),
            pltpu.VMEM((2 * BLOCKS, LANES), F32),
            pltpu.VMEM((2 * BLOCKS, LANES), F32),
            pltpu.VMEM((2 * BLOCKS, LANES), F32),
            pltpu.VMEM((2 * BLOCKS, LANES), F32),
            pltpu.VMEM((2, NP, 8, LANES), F32),
            pltpu.VMEM((2, BLOCKS, LANES), F32),
            pltpu.VMEM((NZ, BLOCKS, LANES), F32),
            pltpu.VMEM((NZ, 2, LANES), F32),
            pltpu.VMEM((NZ, 2, LANES), F32),
            pltpu.VMEM((8, LANES), F32),
            pltpu.VMEM((8, LANES), F32),
            dma((2, 14)), dma((2, 14)), dma((32,)), dma((32,)), dma((2,)), dma((2,)),
            dma((2, NP)), dma((2, NP)), dma((3, NZ)), dma((3, NZ)), dma((6,)), dma((6,)),
        ],
        compiler_params=pltpu.CompilerParams(
            collective_id=0, has_side_effects=True, vmem_limit_bytes=60 * 1024 * 1024
        ),
        name="sinkhorn",
    )(sources, targets, duals_init.reshape(2, LANES))
    return f.reshape(-1), g.reshape(-1)


def solution(mesh):
    return jax.shard_map(
        body,
        mesh=mesh,
        in_specs=(P("blk", None), P(("blk", "tgt"), None), P(("blk", "tgt"))),
        out_specs=(P("blk"), P(("blk", "tgt"))),
        check_vma=False,
    )
```

```python
import functools
import math

import jax
import jax.numpy as jnp
from jax import lax
from jax.experimental import pallas as pl
from jax.experimental.pallas import tpu as pltpu
from jax.sharding import PartitionSpec as P

EPS = 0.05
LOG2E = math.log2(math.e)
SCALE = LOG2E / EPS
MESH = pl.DeviceIdType.MESH
NZ = 8
NP = 16
ROWS = 1024
COLS = 256
BLOCKS = 16
HEAD = 8
D = 128
LANES = 128
CHUNK = 128
CUTS = ((0, HEAD + CHUNK), (HEAD + CHUNK, CHUNK))
F32 = jnp.float32


def lse2(parts):
    high = functools.reduce(jnp.maximum, parts)
    total = functools.reduce(jnp.add, [jnp.exp2(p - high) for p in parts])
    return high + jnp.log2(total)


def kernel(
    log_src, log_dst,
    src_ref, tgt_ref, g0_ref, f_ref, g_ref,
    g0, load_sem, tile, kern, blocks, rows_in, lhs, acc, wide,
    top, row_stat, col_stat, gamma, delta, weight,
    row_buf, pair_buf, z_buf, own_buf, fin_buf, f_own, f_pair,
    ring_send, ring_recv, d2d_send, d2d_recv, x_send, x_recv,
    row_send, row_recv, z_send, z_recv, pair_send, pair_recv,
):
    blk, tgt = lax.axis_index("blk"), lax.axis_index("tgt")
    x_lo, z = blk // NZ, lax.rem(blk, NZ)
    core, x_hi, y = lax.rem(tgt, 2), lax.rem(tgt // 2, 2), tgt // 4
    pair = (blk, tgt + 1 - 2 * core)
    me = x_lo * 8 + tgt // 2

    def on_plane(q):
        return (q // 8) * NZ + z, lax.rem(q, 8) * 2 + core

    def on_ring(other):
        return x_lo * NZ + other, tgt

    def beside(step):
        x = lax.rem(2 * x_hi + x_lo + step + 4, 4)
        return lax.rem(x, 2) * NZ + z, y * 4 + (x // 2) * 2 + x_lo

    swaps = core != x_lo
    left, right = beside(-1), beside(1)
    own = core * NZ + z

    loads = [
        pltpu.make_async_copy(tgt_ref, blocks.at[own, pl.ds(HEAD, COLS), :], load_sem.at[0]),
        pltpu.make_async_copy(g0_ref, g0, load_sem.at[1]),
        pltpu.make_async_copy(src_ref, rows_in, load_sem.at[2]),
    ]
    loads[0].start()
    loads[1].start()

    barrier = pltpu.get_barrier_semaphore()
    for k in range(1, NP):
        pl.semaphore_signal(barrier, inc=1, device_id=on_plane(lax.rem(me + k, NP)), device_id_type=MESH)
    for k in range(1, NZ):
        pl.semaphore_signal(barrier, inc=1, device_id=on_ring(lax.rem(z + k, NZ)), device_id_type=MESH)
    pl.semaphore_signal(barrier, inc=1, device_id=pair, device_id_type=MESH)

    @pl.when(swaps)
    def _():
        for there in (left, right):
            pl.semaphore_signal(barrier, inc=1, device_id=there, device_id_type=MESH)

    @pl.when(jnp.logical_not(swaps))
    def _():
        loads[2].start()

    loads[0].wait()
    loads[1].wait()
    for half in range(2):
        part = blocks[own, HEAD + half * LANES : HEAD + (half + 1) * LANES, :]
        norm = jnp.sum((part * part).T, axis=0, keepdims=True)
        blocks[own, half : half + 1, :] = SCALE * (g0[half : half + 1, :] - norm)

    with jax.named_scope("barrier"):
        pl.semaphore_wait(barrier, NP - 1 + NZ - 1 + 1 + 2 * swaps.astype(jnp.int32))

    def copy(src, dst, send, recv, where):
        return pltpu.make_async_remote_copy(
            src_ref=src, dst_ref=dst, send_sem=send, recv_sem=recv, device_id=where, device_id_type=MESH
        )

    def piece(zb, i):
        start, size = CUTS[i % 2]
        return blocks.at[(NZ if i < 2 else 0) + zb, pl.ds(start, size), :]

    def ring_copy(way, step, i, zb):
        to = on_ring(lax.rem(z + (1 if way == 0 else NZ - 1), NZ))
        slot = 4 * (step - 1) + (i if step < 4 else i % 2)
        return copy(piece(zb, i), piece(zb, i), ring_send, ring_recv.at[way, slot], to)

    def pair_copy(zb, of):
        whole = blocks.at[of * NZ + zb]
        return copy(whole, whole, d2d_send, d2d_recv.at[zb], pair)

    def bytes_of(ref, send, recv):
        return copy(ref, ref, send, recv, pair)

    def goes(way, step, i):
        return step < 4 or (way == 0) == (i < 2)

    def swap_copy(side):
        at = pl.ds(side * (ROWS // 2), ROWS // 2)
        return copy(src_ref.at[at, :], rows_in.at[at, :], x_send.at[side], x_recv.at[side], (left, right)[side])

    carrier = core == 1

    @pl.when(jnp.logical_not(carrier))
    def _():
        pair_copy(z, 0).start()

    @pl.when(carrier)
    def _():
        for i in (0, 1):
            for way in range(2):
                ring_copy(way, 1, i, z).start()
        pair_copy(z, 1).start()

    @pl.when(swaps)
    def _():
        for side in range(2):
            swap_copy(side).start()

    @pl.when(carrier)
    def _():
        pair_copy(z, 0).wait_recv()
        for i in (2, 3):
            for way in range(2):
                ring_copy(way, 1, i, z).start()

    def origin(way, step):
        return lax.rem(z + (NZ - step if way == 0 else step), NZ)

    def receive(step, half):
        @pl.when(carrier)
        def _():
            for i in range(2):
                start, size = CUTS[i]
                for way in range(2):
                    zb = origin(way, step)
                    part = blocks.at[(1 - half) * NZ + zb, pl.ds(start, size), :]
                    to = on_ring(lax.rem(z + (1 if way == 0 else NZ - 1), NZ))
                    slot = 4 * (step - 1) + 2 * half + i
                    came = copy(part, part, ring_send, ring_recv.at[way, slot], to)
                    came.wait_recv()
                    last = step == 3
                    far = 12 + i
                    slot = jnp.where(last, far, slot + 4)

                    @pl.when(jnp.logical_or(jnp.logical_not(last), (half == 0) == (way == 0)))
                    def _():
                        copy(part, part, ring_send, ring_recv.at[way, slot], to).start()

            for way in range(2):
                pair_copy(origin(way, step), 1 - half).start()

    def receive_far():
        @pl.when(carrier)
        def _():
            for i in range(4):
                way = 0 if i < 2 else 1
                zb = origin(way, 4)
                ring_copy(way, 4, i, zb).wait_recv()
                if i % 2 == 1:
                    pair_copy(zb, 1 - way).start()

    def prepare():
        @pl.when(swaps)
        def _():
            for side in range(2):
                swap_copy(side).wait()

        @pl.when(jnp.logical_not(swaps))
        def _():
            loads[2].wait()

        for r in range(ROWS // LANES):
            rows = rows_in[r * LANES : (r + 1) * LANES, :] * (2 * SCALE)
            high = rows.astype(jnp.bfloat16)
            low = (rows - high.astype(F32)).astype(jnp.bfloat16)
            lhs[r * LANES : (r + 1) * LANES, :] = jnp.concatenate([high, low, high, low], axis=1)
        top[...] = jnp.full_like(top, -jnp.inf)
        acc[...] = jnp.zeros_like(acc)

    def scores(zb):
        outs, heads, at = [], [], []
        for which in (core, 1 - core):
            b = which * NZ + zb
            t = blocks[b, HEAD:, :]
            high = t.astype(jnp.bfloat16)
            low = (t - high.astype(F32)).astype(jnp.bfloat16)
            rhs = jnp.concatenate([high, high, low, low], axis=1)
            outs.append(lax.dot_general(lhs[...], rhs, (((1,), (1,)), ((), ())), preferred_element_type=F32))
            heads += [jnp.broadcast_to(blocks[b, h : h + 1, :], (8, LANES)) for h in range(2)]
            at.append(b)
        for k in range(0, ROWS, 8):
            rows = slice(k, k + 8)
            parts = []
            for c in range(4):
                cut = slice((c % 2) * LANES, (c % 2 + 1) * LANES)
                parts.append(outs[c // 2][rows, cut] + heads[c])
                tile[at[c // 2], rows, cut] = parts[c]
            old = top[rows, :]
            new = jnp.maximum(jnp.maximum(parts[0], parts[1]), jnp.maximum(parts[2], parts[3]))
            new = jnp.maximum(old, new)
            top[rows, :] = new
            e = [jnp.exp2(p - new) for p in parts]
            acc[rows, :] = acc[rows, :] * jnp.exp2(old - new) + ((e[0] + e[1]) + (e[2] + e[3]))

    def scores_step(n, carry):
        step = n // 2 + 1
        half = lax.rem(n, 2)

        @pl.when(jnp.logical_and(n >= 2, n < 6))
        def _():
            receive(step, half)

        @pl.when(n == 2 * NZ // 2)
        def _():
            receive_far()

        off = n // 2
        zb = lax.rem(z + jnp.where(half == 0, NZ - off, off), NZ)

        @pl.when(jnp.logical_and(jnp.logical_not(carrier), n == 1))
        def _():
            pair_copy(z, 1).wait_recv()

        @pl.when(jnp.logical_and(jnp.logical_not(carrier), n > 1))
        def _():
            bytes_of(blocks.at[pl.ds(0, 2)], d2d_send, d2d_recv.at[zb]).wait_recv()

        scores(zb)
        return carry

    with jax.named_scope("receive_1"):
        receive(1, 0)
        receive(1, 1)
    with jax.named_scope("prepare"):
        prepare()
    with jax.named_scope("scores"):
        lax.fori_loop(1, NZ + 1, scores_step, 0)

    def spread(row):
        for r in range(ROWS // LANES):
            wide[r * LANES : (r + 1) * LANES, :] = jnp.broadcast_to(row[r : r + 1, :], (LANES, LANES)).T

    x_at = 2 * x_hi + x_lo

    def off_plane(dx, dy):
        x, row = lax.rem(x_at + dx, 4), lax.rem(y + dy, 4)
        return lax.rem(x, 2) * NZ + z, row * 4 + (x // 2) * 2 + core

    def plane_copies(phase):
        slot = row_buf.at[phase, me]
        ways = sorted(
            ((dx, dy) for dx in range(4) for dy in range(4) if dx or dy),
            key=lambda d: -min(d[0], 4 - d[0]) - min(d[1], 4 - d[1]),
        )
        return [
            copy(slot, slot, row_send.at[phase], row_recv.at[phase], off_plane(*d)) for d in ways
        ]

    def plane_bytes(phase):
        return bytes_of(row_buf.at[phase, pl.ds(0, NP - 1)], row_send.at[phase], row_recv.at[phase])

    def across_plane(phase, meanwhile):
        for c in plane_copies(phase):
            c.start()
        meanwhile()

        plane_bytes(phase).wait_recv()

    def plane_sent(phase):
        plane_bytes(phase).wait_send()

    QUAD = 4
    TALL = 256

    def quads(core_of):
        return [core_of * NZ + q * QUAD for q in range(NZ // QUAD)]

    def pick(x, k, h):
        return x[8 * k : 8 * k + 8, h * LANES : (h + 1) * LANES]

    def summed(op, xs):
        return op(functools.reduce(op, xs[0::2]), functools.reduce(op, xs[1::2])) if len(xs) > 1 else xs[0]

    def column_pass(first, into, held, term, op, start):
        def some(r, total):
            at = pl.ds(pl.multiple_of(r * TALL, TALL), TALL)
            w = wide.at[at, :]
            result = []
            for q in range(QUAD):
                view = held.at[first + q, at, :]
                for h in range(2):
                    xs = [term(pick(view, k, h), w[8 * k : 8 * k + 8, :]) for k in range(TALL // 8)]
                    result.append(op(total[2 * q + h], summed(op, xs)))
            return tuple(result)

        total = lax.fori_loop(0, ROWS // TALL, some, (jnp.full((8, LANES), start, F32),) * (2 * QUAD))
        fold = jnp.max if op is jnp.maximum else jnp.sum
        for c in range(2 * QUAD):
            into[pl.ds(2 * first + c, 1), :] = fold(total[c], axis=0, keepdims=True)

    def exp_pass(first):
        tall = 256

        def some(r, total):
            at = pl.ds(pl.multiple_of(r * tall, tall), tall)
            w = wide[at, :]
            result = []
            for q in range(QUAD):
                view = tile.at[first + q, at, :]
                out = kern.at[first + q, at, :]
                for h in range(2):
                    low = gamma[pl.ds(2 * (first + q) + h, 1), :]
                    entry = jnp.exp2((view[:, h * LANES : (h + 1) * LANES] + w) - low)
                    out[:, h * LANES : (h + 1) * LANES] = entry
                    result.append(total[2 * q + h] + jnp.sum(entry.reshape(tall // 8, 8, LANES), axis=0))
            return tuple(result)

        total = lax.fori_loop(0, ROWS // tall, some, (jnp.zeros((8, LANES), F32),) * (2 * QUAD))
        for c in range(2 * QUAD):
            col_stat[pl.ds(2 * first + c, 1), :] = jnp.sum(total[c], axis=0, keepdims=True)

    def row_pass(first, fresh):
        v = [weight[pl.ds(2 * first + c, 1), :] for c in range(2 * QUAD)]

        def some(r, carry):
            at = pl.ds(pl.multiple_of(r * TALL, TALL), TALL)
            views = [kern.at[first + q, at, :] for q in range(QUAD)]
            out = acc.at[at, :]
            for k in range(TALL // 8):
                total = summed(jnp.add, [pick(views[c // 2], k, c % 2) * v[c] for c in range(2 * QUAD)])
                out[8 * k : 8 * k + 8, :] = total if fresh else out[8 * k : 8 * k + 8, :] + total
            return carry

        lax.fori_loop(0, ROWS // TALL, some, 0)

    def halves(step):
        return pl.ds(pl.multiple_of(step * BLOCKS, BLOCKS), BLOCKS)

    def quad_rows(first):
        return pl.ds(pl.multiple_of(2 * first, 8), 8)

    def with_pair(phase, columns, emit):
        swaps_out = []
        for q, first in enumerate(quads(1 - core)):
            columns(first)
            rows = quad_rows(first)
            col_stat[rows, :] = gamma[rows, :] + jnp.log2(col_stat[rows, :])
            to = pair_buf.at[phase, pl.ds(8 * q, 8), :]
            k = 2 * phase + q
            swaps_out.append(copy(col_stat.at[rows, :], to, pair_send.at[k], pair_recv.at[k], pair))
            swaps_out[q].start()
        for q, first in enumerate(quads(core)):
            columns(first)
            rows = quad_rows(first)
            part = gamma[rows, :] + jnp.log2(col_stat[rows, :])
            swaps_out[q].wait()
            emit(q, lse2([part, pair_buf[phase, 8 * q : 8 * q + 8, :]]))

    def ring_copies(q):
        part = z_buf.at[z, pl.ds(8 * q, 8), :]
        return [
            copy(part, part, z_send.at[q], z_recv.at[q], on_ring(lax.rem(z + k, NZ))) for k in (4, 3, 5, 2, 6, 1, 7)
        ]

    def ring_bytes(phase):
        others = pl.ds(0, NZ - 1)
        ref = fin_buf.at[others] if phase == 2 else z_buf.at[others, pl.ds(0, 8), :]
        return bytes_of(ref, z_send.at[phase], z_recv.at[phase])

    with jax.named_scope("row_lse"):
        for r in range(ROWS // LANES):
            at = slice(r * LANES, (r + 1) * LANES)
            lane_top = top[at, :].T
            high = jnp.max(lane_top, axis=0, keepdims=True)
            total = jnp.sum(acc[at, :].T * jnp.exp2(lane_top - high), axis=0, keepdims=True)
            row_buf[0, me, r : r + 1, :] = high + jnp.log2(total)

    def after_gather():
        for r in range(ROWS // LANES):
            rows = rows_in[r * LANES : (r + 1) * LANES, :]
            row_stat[r : r + 1, :] = jnp.sum((rows * rows).T, axis=0, keepdims=True)

        @pl.when(carrier)
        def _():
            bytes_of(blocks.at[pl.ds(0, 14)], ring_send, d2d_recv.at[0]).wait_send()
            bytes_of(blocks.at[pl.ds(0, 15)], d2d_send, d2d_recv.at[0]).wait_send()

        @pl.when(jnp.logical_not(carrier))
        def _():
            pair_copy(z, 0).wait_send()

    with jax.named_scope("plane_0"):
        across_plane(0, after_gather)
    with jax.named_scope("spread"):
        phi = -log_dst - lse2([row_buf[0, q] for q in range(NP)])
        spread(phi)

    def first_columns(first):
        column_pass(first, gamma, tile, jnp.add, jnp.maximum, -jnp.inf)
        exp_pass(first)

    def to_ring(q, joined):
        z_buf[z, 8 * q : 8 * q + 8, :] = joined
        for c in ring_copies(q):
            c.start()

    with jax.named_scope("exp"):
        with_pair(0, first_columns, to_ring)
    with jax.named_scope("ring_0"):
        for q in range(2):
            ring_bytes(q).wait_recv()
    delta[halves(core), :] = -log_src - lse2([z_buf[k] for k in range(NZ)])
    half = delta.at[halves(core), :]
    give = copy(half, half, pair_send.at[4], pair_recv.at[4], pair)
    give.start()

    def weigh(core_of):
        rows = halves(core_of)
        weight[rows, :] = jnp.exp2(delta[rows, :] + gamma[rows, :])

    with jax.named_scope("rows_own"):
        weigh(core)
        for n, first in enumerate(quads(core)):
            row_pass(first, n == 0)
    with jax.named_scope("give"):
        give.wait()
    with jax.named_scope("rows_pair"):
        weigh(1 - core)
        for first in quads(1 - core):
            row_pass(first, False)
        for r in range(ROWS // LANES):
            at = slice(r * LANES, (r + 1) * LANES)
            row_buf[1, me, r : r + 1, :] = jnp.sum(acc[at, :].T, axis=0, keepdims=True)

    def after_ring():
        plane_sent(0)
        for q in range(2):
            ring_bytes(q).wait_send()

    with jax.named_scope("plane_1"):
        across_plane(1, after_ring)
    with jax.named_scope("spread"):
        log_sum = log_dst + jnp.log2(jnp.sum(row_buf[1], axis=0))
        spread(jnp.exp2(-log_sum))
        f_own[...] = row_stat[...] + (phi - log_sum) / SCALE
    hand = copy(f_own, f_pair, pair_send.at[5], pair_recv.at[5], pair)
    hand.start()

    def part_copy(to):
        return copy(own_buf.at[to], fin_buf.at[z], z_send.at[2], z_recv.at[2], on_ring(to))

    def to_owners(q, joined):
        for i in range(NZ // 2):
            to = NZ // 2 * q + i
            part = joined[2 * i : 2 * i + 2, :]
            own_buf[to] = part

            @pl.when(z == to)
            def _():
                fin_buf[to] = part

            @pl.when(z != to)
            def _():
                part_copy(to).start()

    with jax.named_scope("cols"):
        with_pair(1, lambda first: column_pass(first, col_stat, kern, jnp.multiply, jnp.add, 0.0), to_owners)
    with jax.named_scope("ring_1"):
        plane_sent(1)
        hand.wait()
        f_ref[...] = jnp.where(swaps, f_pair[...], f_own[...])
        ring_bytes(2).wait_recv()
    g_ref[...] = g0[...] - (log_src + lse2([fin_buf[k] for k in range(NZ)])) / SCALE
    ring_bytes(2).wait_send()


def body(sources, targets, duals_init):
    n_src = sources.shape[0] * lax.axis_size("blk")
    n_dst = targets.shape[0] * lax.axis_size("blk") * lax.axis_size("tgt")
    vmem = pl.BlockSpec(memory_space=pltpu.VMEM)
    dma = pltpu.SemaphoreType.DMA
    f, g = pl.pallas_call(
        functools.partial(kernel, math.log2(n_src), math.log2(n_dst)),
        out_shape=(pltpu.VMEM((8, LANES), F32), pltpu.VMEM((2, LANES), F32)),
        in_specs=[pl.BlockSpec(memory_space=pl.ANY)] * 3,
        out_specs=(vmem, vmem),
        scratch_shapes=[
            pltpu.VMEM((2, LANES), F32),
            dma((3,)),
            pltpu.VMEM((BLOCKS, ROWS, COLS), F32),
            pltpu.VMEM((BLOCKS, ROWS, COLS), F32),
            pltpu.VMEM((BLOCKS, HEAD + COLS, D), F32),
            pltpu.VMEM((ROWS, D), F32),
            pltpu.VMEM((ROWS, 4 * D), jnp.bfloat16),
            pltpu.VMEM((ROWS, LANES), F32),
            pltpu.VMEM((ROWS, LANES), F32),
            pltpu.VMEM((ROWS, LANES), F32),
            pltpu.VMEM((8, LANES), F32),
            pltpu.VMEM((2 * BLOCKS, LANES), F32),
            pltpu.VMEM((2 * BLOCKS, LANES), F32),
            pltpu.VMEM((2 * BLOCKS, LANES), F32),
            pltpu.VMEM((2 * BLOCKS, LANES), F32),
            pltpu.VMEM((2, NP, 8, LANES), F32),
            pltpu.VMEM((2, BLOCKS, LANES), F32),
            pltpu.VMEM((NZ, BLOCKS, LANES), F32),
            pltpu.VMEM((NZ, 2, LANES), F32),
            pltpu.VMEM((NZ, 2, LANES), F32),
            pltpu.VMEM((8, LANES), F32),
            pltpu.VMEM((8, LANES), F32),
            dma, dma((2, 14)), dma, dma((NZ,)), dma((2,)), dma((2,)),
            dma((2,)), dma((2,)), dma((3,)), dma((3,)), dma((6,)), dma((6,)),
        ],
        compiler_params=pltpu.CompilerParams(
            collective_id=0, has_side_effects=True, vmem_limit_bytes=60 * 1024 * 1024
        ),
        name="sinkhorn",
    )(sources, targets, duals_init.reshape(2, LANES))
    return f.reshape(-1), g.reshape(-1)


def solution(mesh):
    return jax.shard_map(
        body,
        mesh=mesh,
        in_specs=(P("blk", None), P(("blk", "tgt"), None), P(("blk", "tgt"))),
        out_specs=(P("blk"), P(("blk", "tgt"))),
        check_vma=False,
    )
```

```python
import functools
import math

import jax
import jax.numpy as jnp
from jax import lax
from jax.experimental import pallas as pl
from jax.experimental.pallas import tpu as pltpu
from jax.sharding import PartitionSpec as P

EPS = 0.05
LOG2E = math.log2(math.e)
SCALE = LOG2E / EPS
MESH = pl.DeviceIdType.MESH
NZ = 8
NP = 16
ROWS = 1024
COLS = 256
BLOCKS = 16
HEAD = 8
D = 128
LANES = 128
CHUNK = 128
CUTS = ((0, HEAD + CHUNK), (HEAD + CHUNK, CHUNK))
F32 = jnp.float32


def lse2(parts):
    high = functools.reduce(jnp.maximum, parts)
    total = functools.reduce(jnp.add, [jnp.exp2(p - high) for p in parts])
    return high + jnp.log2(total)


def kernel(
    log_src, log_dst,
    src_ref, tgt_ref, g0_ref, f_ref, g_ref,
    g0, load_sem, tile, kern, blocks, rows_in, lhs, acc, wide,
    top, row_stat, col_stat, gamma, delta, weight,
    row_buf, pair_buf, z_buf, own_buf, fin_buf, f_own, f_pair,
    met, ring_send, ring_recv, d2d_send, d2d_recv, x_send, x_recv,
    row_send, row_recv, z_send, z_recv, pair_send, pair_recv,
):
    blk, tgt = lax.axis_index("blk"), lax.axis_index("tgt")
    x_lo, z = blk // NZ, lax.rem(blk, NZ)
    core, x_hi, y = lax.rem(tgt, 2), lax.rem(tgt // 2, 2), tgt // 4
    pair = (blk, tgt + 1 - 2 * core)
    me = x_lo * 8 + tgt // 2

    x_at = 2 * x_hi + x_lo

    def off_plane(dx, dy):
        x, row = lax.rem(x_at + dx, 4), lax.rem(y + dy, 4)
        return lax.rem(x, 2) * NZ + z, row * 4 + (x // 2) * 2 + core

    def on_ring(other):
        return x_lo * NZ + other, tgt

    def beside(step):
        x = lax.rem(2 * x_hi + x_lo + step + 4, 4)
        return lax.rem(x, 2) * NZ + z, y * 4 + (x // 2) * 2 + x_lo

    swaps = core != x_lo
    left, right = beside(-1), beside(1)
    own = core * NZ + z

    loads = [
        pltpu.make_async_copy(tgt_ref, blocks.at[own, pl.ds(HEAD, COLS), :], load_sem.at[0]),
        pltpu.make_async_copy(g0_ref, g0, load_sem.at[1]),
        pltpu.make_async_copy(src_ref, rows_in, load_sem.at[2]),
    ]
    loads[0].start()
    loads[1].start()

    barrier = pltpu.get_barrier_semaphore()
    around = [off_plane(dx, dy) for dx, dy in ((1, 0), (3, 0), (0, 1), (0, 3))]
    for there in (on_ring(lax.rem(z + 1, NZ)), on_ring(lax.rem(z + NZ - 1, NZ)), pair, *around):
        pl.semaphore_signal(barrier, inc=1, device_id=there, device_id_type=MESH)

    @pl.when(swaps)
    def _():
        for there in (left, right):
            pl.semaphore_signal(barrier, inc=1, device_id=there, device_id_type=MESH)

    @pl.when(jnp.logical_not(swaps))
    def _():
        loads[2].start()

    loads[0].wait()
    loads[1].wait()
    for half in range(2):
        part = blocks[own, HEAD + half * LANES : HEAD + (half + 1) * LANES, :]
        norm = jnp.sum((part * part).T, axis=0, keepdims=True)
        blocks[own, half : half + 1, :] = SCALE * (g0[half : half + 1, :] - norm)

    with jax.named_scope("barrier"):
        pl.semaphore_wait(barrier, 7 + 2 * swaps.astype(jnp.int32))

    def copy(src, dst, send, recv, where):
        return pltpu.make_async_remote_copy(
            src_ref=src, dst_ref=dst, send_sem=send, recv_sem=recv, device_id=where, device_id_type=MESH
        )

    def piece(zb, i):
        start, size = CUTS[i % 2]
        return blocks.at[(NZ if i < 2 else 0) + zb, pl.ds(start, size), :]

    def ring_copy(way, step, i, zb):
        to = on_ring(lax.rem(z + (1 if way == 0 else NZ - 1), NZ))
        slot = 4 * (step - 1) + (i if step < 4 else i % 2)
        return copy(piece(zb, i), piece(zb, i), ring_send, ring_recv.at[way, slot], to)

    def pair_copy(zb, of):
        whole = blocks.at[of * NZ + zb]
        return copy(whole, whole, d2d_send, d2d_recv.at[zb], pair)

    def bytes_of(ref, send, recv):
        return copy(ref, ref, send, recv, pair)

    def goes(way, step, i):
        return step < 4 or (way == 0) == (i < 2)

    def swap_copy(side):
        at = pl.ds(side * (ROWS // 2), ROWS // 2)
        return copy(src_ref.at[at, :], rows_in.at[at, :], x_send.at[side], x_recv.at[side], (left, right)[side])

    carrier = core == 1

    @pl.when(jnp.logical_not(carrier))
    def _():
        pair_copy(z, 0).start()

    @pl.when(carrier)
    def _():
        for i in (0, 1):
            for way in range(2):
                ring_copy(way, 1, i, z).start()
        pair_copy(z, 1).start()

    @pl.when(swaps)
    def _():
        for side in range(2):
            swap_copy(side).start()

    @pl.when(carrier)
    def _():
        pair_copy(z, 0).wait_recv()
        for i in (2, 3):
            for way in range(2):
                ring_copy(way, 1, i, z).start()

    def greet(r):
        for there in around:
            pl.semaphore_signal(met.at[r], inc=1, device_id=there, device_id_type=MESH)

    def hear(r):
        pl.semaphore_wait(met.at[r], len(around))

    greet(0)

    def origin(way, step):
        return lax.rem(z + (NZ - step if way == 0 else step), NZ)

    def receive(step, half):
        @pl.when(carrier)
        def _():
            for i in range(2):
                start, size = CUTS[i]
                for way in range(2):
                    zb = origin(way, step)
                    part = blocks.at[(1 - half) * NZ + zb, pl.ds(start, size), :]
                    to = on_ring(lax.rem(z + (1 if way == 0 else NZ - 1), NZ))
                    slot = 4 * (step - 1) + 2 * half + i
                    came = copy(part, part, ring_send, ring_recv.at[way, slot], to)
                    came.wait_recv()
                    last = step == 3
                    far = 12 + i
                    slot = jnp.where(last, far, slot + 4)

                    @pl.when(jnp.logical_or(jnp.logical_not(last), (half == 0) == (way == 0)))
                    def _():
                        copy(part, part, ring_send, ring_recv.at[way, slot], to).start()

            for way in range(2):
                pair_copy(origin(way, step), 1 - half).start()

    def receive_far():
        @pl.when(carrier)
        def _():
            for i in range(4):
                way = 0 if i < 2 else 1
                zb = origin(way, 4)
                ring_copy(way, 4, i, zb).wait_recv()
                if i % 2 == 1:
                    pair_copy(zb, 1 - way).start()

    def prepare():
        @pl.when(swaps)
        def _():
            for side in range(2):
                swap_copy(side).wait()

        @pl.when(jnp.logical_not(swaps))
        def _():
            loads[2].wait()

        for r in range(ROWS // LANES):
            rows = rows_in[r * LANES : (r + 1) * LANES, :] * (2 * SCALE)
            high = rows.astype(jnp.bfloat16)
            low = (rows - high.astype(F32)).astype(jnp.bfloat16)
            lhs[r * LANES : (r + 1) * LANES, :] = jnp.concatenate([high, low, high, low], axis=1)
        top[...] = jnp.full_like(top, -jnp.inf)
        acc[...] = jnp.zeros_like(acc)

    def scores(zb):
        outs, heads, at = [], [], []
        for which in (core, 1 - core):
            b = which * NZ + zb
            t = blocks[b, HEAD:, :]
            high = t.astype(jnp.bfloat16)
            low = (t - high.astype(F32)).astype(jnp.bfloat16)
            rhs = jnp.concatenate([high, high, low, low], axis=1)
            outs.append(lax.dot_general(lhs[...], rhs, (((1,), (1,)), ((), ())), preferred_element_type=F32))
            heads += [jnp.broadcast_to(blocks[b, h : h + 1, :], (8, LANES)) for h in range(2)]
            at.append(b)
        for k in range(0, ROWS, 8):
            rows = slice(k, k + 8)
            parts = []
            for c in range(4):
                cut = slice((c % 2) * LANES, (c % 2 + 1) * LANES)
                parts.append(outs[c // 2][rows, cut] + heads[c])
                tile[at[c // 2], rows, cut] = parts[c]
            old = top[rows, :]
            new = jnp.maximum(jnp.maximum(parts[0], parts[1]), jnp.maximum(parts[2], parts[3]))
            new = jnp.maximum(old, new)
            top[rows, :] = new
            e = [jnp.exp2(p - new) for p in parts]
            acc[rows, :] = acc[rows, :] * jnp.exp2(old - new) + ((e[0] + e[1]) + (e[2] + e[3]))

    def scores_step(n, carry):
        step = n // 2 + 1
        half = lax.rem(n, 2)

        @pl.when(jnp.logical_and(n >= 2, n < 6))
        def _():
            receive(step, half)

        @pl.when(n == 2 * NZ // 2)
        def _():
            receive_far()

        off = n // 2
        zb = lax.rem(z + jnp.where(half == 0, NZ - off, off), NZ)

        @pl.when(jnp.logical_and(jnp.logical_not(carrier), n == 1))
        def _():
            pair_copy(z, 1).wait_recv()

        @pl.when(jnp.logical_and(jnp.logical_not(carrier), n > 1))
        def _():
            bytes_of(blocks.at[pl.ds(0, 2)], d2d_send, d2d_recv.at[zb]).wait_recv()

        scores(zb)

        @pl.when(jnp.logical_or(n == 1, n == 3))
        def _():
            hear(n // 2)
            greet(n // 2 + 1)

        return carry

    with jax.named_scope("receive_1"):
        receive(1, 0)
        receive(1, 1)
    with jax.named_scope("prepare"):
        prepare()
    with jax.named_scope("scores"):
        lax.fori_loop(1, NZ + 1, scores_step, 0)
        hear(2)

    def spread(row):
        for r in range(ROWS // LANES):
            wide[r * LANES : (r + 1) * LANES, :] = jnp.broadcast_to(row[r : r + 1, :], (LANES, LANES)).T

    def plane_copies(phase):
        slot = row_buf.at[phase, me]
        ways = sorted(
            ((dx, dy) for dx in range(4) for dy in range(4) if dx or dy),
            key=lambda d: -min(d[0], 4 - d[0]) - min(d[1], 4 - d[1]),
        )
        return [
            copy(slot, slot, row_send.at[phase], row_recv.at[phase], off_plane(*d)) for d in ways
        ]

    def plane_bytes(phase):
        return bytes_of(row_buf.at[phase, pl.ds(0, NP - 1)], row_send.at[phase], row_recv.at[phase])

    def across_plane(phase, meanwhile):
        for c in plane_copies(phase):
            c.start()
        meanwhile()

        plane_bytes(phase).wait_recv()

    def plane_sent(phase):
        plane_bytes(phase).wait_send()

    QUAD = 4
    TALL = 256

    def quads(core_of):
        return [core_of * NZ + q * QUAD for q in range(NZ // QUAD)]

    def pick(x, k, h):
        return x[8 * k : 8 * k + 8, h * LANES : (h + 1) * LANES]

    def summed(op, xs):
        return op(functools.reduce(op, xs[0::2]), functools.reduce(op, xs[1::2])) if len(xs) > 1 else xs[0]

    def column_pass(first, into, held, term, op, start):
        def some(r, total):
            at = pl.ds(pl.multiple_of(r * TALL, TALL), TALL)
            w = wide.at[at, :]
            result = []
            for q in range(QUAD):
                view = held.at[first + q, at, :]
                for h in range(2):
                    xs = [term(pick(view, k, h), w[8 * k : 8 * k + 8, :]) for k in range(TALL // 8)]
                    result.append(op(total[2 * q + h], summed(op, xs)))
            return tuple(result)

        total = lax.fori_loop(0, ROWS // TALL, some, (jnp.full((8, LANES), start, F32),) * (2 * QUAD))
        fold = jnp.max if op is jnp.maximum else jnp.sum
        for c in range(2 * QUAD):
            into[pl.ds(2 * first + c, 1), :] = fold(total[c], axis=0, keepdims=True)

    def exp_pass(first):
        tall = 256

        def some(r, total):
            at = pl.ds(pl.multiple_of(r * tall, tall), tall)
            w = wide[at, :]
            result = []
            for q in range(QUAD):
                view = tile.at[first + q, at, :]
                out = kern.at[first + q, at, :]
                for h in range(2):
                    low = gamma[pl.ds(2 * (first + q) + h, 1), :]
                    entry = jnp.exp2((view[:, h * LANES : (h + 1) * LANES] + w) - low)
                    out[:, h * LANES : (h + 1) * LANES] = entry
                    result.append(total[2 * q + h] + jnp.sum(entry.reshape(tall // 8, 8, LANES), axis=0))
            return tuple(result)

        total = lax.fori_loop(0, ROWS // tall, some, (jnp.zeros((8, LANES), F32),) * (2 * QUAD))
        for c in range(2 * QUAD):
            col_stat[pl.ds(2 * first + c, 1), :] = jnp.sum(total[c], axis=0, keepdims=True)

    def row_pass(first, fresh):
        v = [weight[pl.ds(2 * first + c, 1), :] for c in range(2 * QUAD)]

        def some(r, carry):
            at = pl.ds(pl.multiple_of(r * TALL, TALL), TALL)
            views = [kern.at[first + q, at, :] for q in range(QUAD)]
            out = acc.at[at, :]
            for k in range(TALL // 8):
                total = summed(jnp.add, [pick(views[c // 2], k, c % 2) * v[c] for c in range(2 * QUAD)])
                out[8 * k : 8 * k + 8, :] = total if fresh else out[8 * k : 8 * k + 8, :] + total
            return carry

        lax.fori_loop(0, ROWS // TALL, some, 0)

    def halves(step):
        return pl.ds(pl.multiple_of(step * BLOCKS, BLOCKS), BLOCKS)

    def quad_rows(first):
        return pl.ds(pl.multiple_of(2 * first, 8), 8)

    def with_pair(phase, columns, emit):
        swaps_out = []
        for q, first in enumerate(quads(1 - core)):
            columns(first)
            rows = quad_rows(first)
            col_stat[rows, :] = gamma[rows, :] + jnp.log2(col_stat[rows, :])
            to = pair_buf.at[phase, pl.ds(8 * q, 8), :]
            k = 2 * phase + q
            swaps_out.append(copy(col_stat.at[rows, :], to, pair_send.at[k], pair_recv.at[k], pair))
            swaps_out[q].start()
        for q, first in enumerate(quads(core)):
            columns(first)
            rows = quad_rows(first)
            part = gamma[rows, :] + jnp.log2(col_stat[rows, :])
            swaps_out[q].wait()
            emit(q, lse2([part, pair_buf[phase, 8 * q : 8 * q + 8, :]]))

    def ring_copies(q):
        part = z_buf.at[z, pl.ds(8 * q, 8), :]
        return [
            copy(part, part, z_send.at[q], z_recv.at[q], on_ring(lax.rem(z + k, NZ))) for k in (4, 3, 5, 2, 6, 1, 7)
        ]

    def ring_bytes(phase):
        others = pl.ds(0, NZ - 1)
        ref = fin_buf.at[others] if phase == 2 else z_buf.at[others, pl.ds(0, 8), :]
        return bytes_of(ref, z_send.at[phase], z_recv.at[phase])

    with jax.named_scope("row_lse"):
        for r in range(ROWS // LANES):
            at = slice(r * LANES, (r + 1) * LANES)
            lane_top = top[at, :].T
            high = jnp.max(lane_top, axis=0, keepdims=True)
            total = jnp.sum(acc[at, :].T * jnp.exp2(lane_top - high), axis=0, keepdims=True)
            row_buf[0, me, r : r + 1, :] = high + jnp.log2(total)

    def after_gather():
        for r in range(ROWS // LANES):
            rows = rows_in[r * LANES : (r + 1) * LANES, :]
            row_stat[r : r + 1, :] = jnp.sum((rows * rows).T, axis=0, keepdims=True)

        @pl.when(carrier)
        def _():
            bytes_of(blocks.at[pl.ds(0, 14)], ring_send, d2d_recv.at[0]).wait_send()
            bytes_of(blocks.at[pl.ds(0, 15)], d2d_send, d2d_recv.at[0]).wait_send()

        @pl.when(jnp.logical_not(carrier))
        def _():
            pair_copy(z, 0).wait_send()

    with jax.named_scope("plane_0"):
        across_plane(0, after_gather)
    with jax.named_scope("spread"):
        phi = -log_dst - lse2([row_buf[0, q] for q in range(NP)])
        spread(phi)

    def first_columns(first):
        column_pass(first, gamma, tile, jnp.add, jnp.maximum, -jnp.inf)
        exp_pass(first)

    def to_ring(q, joined):
        z_buf[z, 8 * q : 8 * q + 8, :] = joined
        for c in ring_copies(q):
            c.start()

    with jax.named_scope("exp"):
        with_pair(0, first_columns, to_ring)
    with jax.named_scope("ring_0"):
        for q in range(2):
            ring_bytes(q).wait_recv()
    delta[halves(core), :] = -log_src - lse2([z_buf[k] for k in range(NZ)])
    half = delta.at[halves(core), :]
    give = copy(half, half, pair_send.at[4], pair_recv.at[4], pair)
    give.start()

    def weigh(core_of):
        rows = halves(core_of)
        weight[rows, :] = jnp.exp2(delta[rows, :] + gamma[rows, :])

    with jax.named_scope("rows_own"):
        weigh(core)
        for n, first in enumerate(quads(core)):
            row_pass(first, n == 0)
    with jax.named_scope("give"):
        give.wait()
    with jax.named_scope("rows_pair"):
        weigh(1 - core)
        for first in quads(1 - core):
            row_pass(first, False)
        for r in range(ROWS // LANES):
            at = slice(r * LANES, (r + 1) * LANES)
            row_buf[1, me, r : r + 1, :] = jnp.sum(acc[at, :].T, axis=0, keepdims=True)

    def after_ring():
        plane_sent(0)
        for q in range(2):
            ring_bytes(q).wait_send()

    with jax.named_scope("plane_1"):
        across_plane(1, after_ring)
    with jax.named_scope("spread"):
        log_sum = log_dst + jnp.log2(jnp.sum(row_buf[1], axis=0))
        spread(jnp.exp2(-log_sum))
        f_own[...] = row_stat[...] + (phi - log_sum) / SCALE
    hand = copy(f_own, f_pair, pair_send.at[5], pair_recv.at[5], pair)
    hand.start()

    def part_copy(to):
        return copy(own_buf.at[to], fin_buf.at[z], z_send.at[2], z_recv.at[2], on_ring(to))

    def to_owners(q, joined):
        for i in range(NZ // 2):
            to = NZ // 2 * q + i
            part = joined[2 * i : 2 * i + 2, :]
            own_buf[to] = part

            @pl.when(z == to)
            def _():
                fin_buf[to] = part

            @pl.when(z != to)
            def _():
                part_copy(to).start()

    with jax.named_scope("cols"):
        with_pair(1, lambda first: column_pass(first, col_stat, kern, jnp.multiply, jnp.add, 0.0), to_owners)
    with jax.named_scope("ring_1"):
        plane_sent(1)
        hand.wait()
        f_ref[...] = jnp.where(swaps, f_pair[...], f_own[...])
        ring_bytes(2).wait_recv()
    g_ref[...] = g0[...] - (log_src + lse2([fin_buf[k] for k in range(NZ)])) / SCALE
    ring_bytes(2).wait_send()


def body(sources, targets, duals_init):
    n_src = sources.shape[0] * lax.axis_size("blk")
    n_dst = targets.shape[0] * lax.axis_size("blk") * lax.axis_size("tgt")
    vmem = pl.BlockSpec(memory_space=pltpu.VMEM)
    dma = pltpu.SemaphoreType.DMA
    f, g = pl.pallas_call(
        functools.partial(kernel, math.log2(n_src), math.log2(n_dst)),
        out_shape=(pltpu.VMEM((8, LANES), F32), pltpu.VMEM((2, LANES), F32)),
        in_specs=[pl.BlockSpec(memory_space=pl.ANY)] * 3,
        out_specs=(vmem, vmem),
        scratch_shapes=[
            pltpu.VMEM((2, LANES), F32),
            dma((3,)),
            pltpu.VMEM((BLOCKS, ROWS, COLS), F32),
            pltpu.VMEM((BLOCKS, ROWS, COLS), F32),
            pltpu.VMEM((BLOCKS, HEAD + COLS, D), F32),
            pltpu.VMEM((ROWS, D), F32),
            pltpu.VMEM((ROWS, 4 * D), jnp.bfloat16),
            pltpu.VMEM((ROWS, LANES), F32),
            pltpu.VMEM((ROWS, LANES), F32),
            pltpu.VMEM((ROWS, LANES), F32),
            pltpu.VMEM((8, LANES), F32),
            pltpu.VMEM((2 * BLOCKS, LANES), F32),
            pltpu.VMEM((2 * BLOCKS, LANES), F32),
            pltpu.VMEM((2 * BLOCKS, LANES), F32),
            pltpu.VMEM((2 * BLOCKS, LANES), F32),
            pltpu.VMEM((2, NP, 8, LANES), F32),
            pltpu.VMEM((2, BLOCKS, LANES), F32),
            pltpu.VMEM((NZ, BLOCKS, LANES), F32),
            pltpu.VMEM((NZ, 2, LANES), F32),
            pltpu.VMEM((NZ, 2, LANES), F32),
            pltpu.VMEM((8, LANES), F32),
            pltpu.VMEM((8, LANES), F32),
            pltpu.SemaphoreType.REGULAR((3,)), dma, dma((2, 14)), dma, dma((NZ,)), dma((2,)), dma((2,)),
            dma((2,)), dma((2,)), dma((3,)), dma((3,)), dma((6,)), dma((6,)),
        ],
        compiler_params=pltpu.CompilerParams(
            collective_id=0, has_side_effects=True, vmem_limit_bytes=60 * 1024 * 1024
        ),
        name="sinkhorn",
    )(sources, targets, duals_init.reshape(2, LANES))
    return f.reshape(-1), g.reshape(-1)


def solution(mesh):
    return jax.shard_map(
        body,
        mesh=mesh,
        in_specs=(P("blk", None), P(("blk", "tgt"), None), P(("blk", "tgt"))),
        out_specs=(P("blk"), P(("blk", "tgt"))),
        check_vma=False,
    )
```

```python
import functools
import math

import jax
import jax.numpy as jnp
from jax import lax
from jax.experimental import pallas as pl
from jax.experimental.pallas import tpu as pltpu
from jax.sharding import PartitionSpec as P

EPS = 0.05
LOG2E = math.log2(math.e)
SCALE = LOG2E / EPS
MESH = pl.DeviceIdType.MESH
NZ = 8
NP = 16
ROWS = 1024
COLS = 256
BLOCKS = 16
HEAD = 8
D = 128
LANES = 128
CHUNK = 128
CUTS = ((0, HEAD + CHUNK), (HEAD + CHUNK, CHUNK))
F32 = jnp.float32


def lse2(parts):
    high = functools.reduce(jnp.maximum, parts)
    total = functools.reduce(jnp.add, [jnp.exp2(p - high) for p in parts])
    return high + jnp.log2(total)


def kernel(
    log_src, log_dst,
    src_ref, tgt_ref, g0_ref, f_ref, g_ref,
    g0, load_sem, tile, kern, blocks, rows_in, lhs, acc, wide,
    top, row_stat, col_stat, gamma, delta, weight,
    row_buf, pair_buf, z_buf, own_buf, fin_buf, f_own, f_pair,
    met, ring_send, ring_recv, d2d_send, d2d_recv, x_send, x_recv,
    row_send, row_recv, z_send, z_recv, pair_send, pair_recv,
):
    blk, tgt = lax.axis_index("blk"), lax.axis_index("tgt")
    x_lo, z = blk // NZ, lax.rem(blk, NZ)
    core, x_hi, y = lax.rem(tgt, 2), lax.rem(tgt // 2, 2), tgt // 4
    pair = (blk, tgt + 1 - 2 * core)
    me = x_lo * 8 + tgt // 2

    x_at = 2 * x_hi + x_lo

    def off_plane(dx, dy):
        x, row = lax.rem(x_at + dx, 4), lax.rem(y + dy, 4)
        return lax.rem(x, 2) * NZ + z, row * 4 + (x // 2) * 2 + core

    def same_rows(dx, dy):
        blk_there, tgt_there = off_plane(dx, dy)
        return blk_there, tgt_there if dx % 2 == 0 else tgt_there + 1 - 2 * core

    def on_ring(other):
        return x_lo * NZ + other, tgt

    carrier = core == 1
    swaps = core == 0
    left, right = off_plane(3, 0), off_plane(1, 0)
    own = core * NZ + z

    loads = [
        pltpu.make_async_copy(tgt_ref, blocks.at[own, pl.ds(HEAD, COLS), :], load_sem.at[0]),
        pltpu.make_async_copy(g0_ref, g0, load_sem.at[1]),
        pltpu.make_async_copy(src_ref, rows_in, load_sem.at[2]),
    ]
    loads[0].start()
    loads[1].start()

    barrier = pltpu.get_barrier_semaphore()
    around = [off_plane(dx, dy) for dx, dy in ((1, 0), (3, 0), (0, 1), (0, 3))]
    for there in (on_ring(lax.rem(z + 1, NZ)), on_ring(lax.rem(z + NZ - 1, NZ)), pair, *around):
        pl.semaphore_signal(barrier, inc=1, device_id=there, device_id_type=MESH)

    @pl.when(jnp.logical_not(swaps))
    def _():
        loads[2].start()

    loads[0].wait()
    loads[1].wait()
    for half in range(2):
        part = blocks[own, HEAD + half * LANES : HEAD + (half + 1) * LANES, :]
        norm = jnp.sum((part * part).T, axis=0, keepdims=True)
        blocks[own, half : half + 1, :] = SCALE * (g0[half : half + 1, :] - norm)

    with jax.named_scope("barrier"):
        pl.semaphore_wait(barrier, 7)

    def copy(src, dst, send, recv, where):
        return pltpu.make_async_remote_copy(
            src_ref=src, dst_ref=dst, send_sem=send, recv_sem=recv, device_id=where, device_id_type=MESH
        )

    def piece(zb, i):
        start, size = CUTS[i % 2]
        return blocks.at[(NZ if i < 2 else 0) + zb, pl.ds(start, size), :]

    def ring_copy(way, step, i, zb):
        to = on_ring(lax.rem(z + (1 if way == 0 else NZ - 1), NZ))
        slot = 4 * (step - 1) + (i if step < 4 else i // 2)
        return copy(piece(zb, i), piece(zb, i), ring_send, ring_recv.at[way, slot], to)

    def pair_copy(zb, of):
        whole = blocks.at[of * NZ + zb]
        return copy(whole, whole, d2d_send, d2d_recv.at[zb], pair)

    def bytes_of(ref, send, recv):
        return copy(ref, ref, send, recv, pair)

    def goes(way, step, i):
        return step < 4 or i % 2 == way

    def swap_copy(side):
        at = pl.ds(side * (ROWS // 2), ROWS // 2)
        return copy(src_ref.at[at, :], rows_in.at[at, :], x_send.at[side], x_recv.at[side], (left, right)[side])

    @pl.when(jnp.logical_not(carrier))
    def _():
        pair_copy(z, 0).start()

    @pl.when(carrier)
    def _():
        for i in (0, 1):
            for way in range(2):
                ring_copy(way, 1, i, z).start()
        pair_copy(z, 1).start()

    @pl.when(swaps)
    def _():
        for side in range(2):
            swap_copy(side).start()

    @pl.when(carrier)
    def _():
        pair_copy(z, 0).wait_recv()
        for i in (2, 3):
            for way in range(2):
                ring_copy(way, 1, i, z).start()

    def greet(r):
        for there in around:
            pl.semaphore_signal(met.at[r], inc=1, device_id=there, device_id_type=MESH)

    def hear(r):
        pl.semaphore_wait(met.at[r], len(around))

    greet(0)

    def origin(way, step):
        return lax.rem(z + (NZ - step if way == 0 else step), NZ)

    def receive(step, half):
        @pl.when(carrier)
        def _():
            for i in range(2):
                start, size = CUTS[i]
                for way in range(2):
                    zb = origin(way, step)
                    part = blocks.at[(1 - half) * NZ + zb, pl.ds(start, size), :]
                    to = on_ring(lax.rem(z + (1 if way == 0 else NZ - 1), NZ))
                    slot = 4 * (step - 1) + 2 * half + i
                    came = copy(part, part, ring_send, ring_recv.at[way, slot], to)
                    came.wait_recv()
                    last = step == 3
                    slot = jnp.where(last, 12 + half, slot + 4)

                    @pl.when(jnp.logical_or(jnp.logical_not(last), i == way))
                    def _():
                        copy(part, part, ring_send, ring_recv.at[way, slot], to).start()

            for way in range(2):
                pair_copy(origin(way, step), 1 - half).start()

    def receive_far():
        @pl.when(carrier)
        def _():
            far = origin(0, 4)
            for half in range(2):
                for way in range(2):
                    ring_copy(way, 4, 2 * half + way, far).wait_recv()
                pair_copy(far, 1 - half).start()

    def prepare():
        @pl.when(swaps)
        def _():
            for side in range(2):
                swap_copy(side).wait()

        @pl.when(jnp.logical_not(swaps))
        def _():
            loads[2].wait()

        for r in range(ROWS // LANES):
            rows = rows_in[r * LANES : (r + 1) * LANES, :] * (2 * SCALE)
            high = rows.astype(jnp.bfloat16)
            low = (rows - high.astype(F32)).astype(jnp.bfloat16)
            lhs[r * LANES : (r + 1) * LANES, :] = jnp.concatenate([high, low, high, low], axis=1)
        top[...] = jnp.full_like(top, -jnp.inf)
        acc[...] = jnp.zeros_like(acc)

    def scores(zb):
        outs, heads, at = [], [], []
        for which in (core, 1 - core):
            b = which * NZ + zb
            t = blocks[b, HEAD:, :]
            high = t.astype(jnp.bfloat16)
            low = (t - high.astype(F32)).astype(jnp.bfloat16)
            rhs = jnp.concatenate([high, high, low, low], axis=1)
            outs.append(lax.dot_general(lhs[...], rhs, (((1,), (1,)), ((), ())), preferred_element_type=F32))
            heads += [jnp.broadcast_to(blocks[b, h : h + 1, :], (8, LANES)) for h in range(2)]
            at.append(b)
        for k in range(0, ROWS, 8):
            rows = slice(k, k + 8)
            parts = []
            for c in range(4):
                cut = slice((c % 2) * LANES, (c % 2 + 1) * LANES)
                parts.append(outs[c // 2][rows, cut] + heads[c])
                tile[at[c // 2], rows, cut] = parts[c]
            old = top[rows, :]
            new = jnp.maximum(jnp.maximum(parts[0], parts[1]), jnp.maximum(parts[2], parts[3]))
            new = jnp.maximum(old, new)
            top[rows, :] = new
            e = [jnp.exp2(p - new) for p in parts]
            acc[rows, :] = acc[rows, :] * jnp.exp2(old - new) + ((e[0] + e[1]) + (e[2] + e[3]))

    def scores_step(n, carry):
        half = lax.rem(n, 2)

        @pl.when(n == 2)
        def _():
            receive(1, 0)
            receive(1, 1)

        @pl.when(jnp.logical_and(n >= 3, n < 7))
        def _():
            receive((n + 1) // 2, 1 - half)

        @pl.when(n == NZ)
        def _():
            receive_far()

        off = n // 2
        zb = lax.rem(z + jnp.where(half == 0, NZ - off, off), NZ)

        @pl.when(jnp.logical_and(jnp.logical_not(carrier), n == 1))
        def _():
            pair_copy(z, 1).wait_recv()

        @pl.when(jnp.logical_and(jnp.logical_not(carrier), n > 1))
        def _():
            bytes_of(blocks.at[pl.ds(0, 2)], d2d_send, d2d_recv.at[zb]).wait_recv()

        scores(zb)

        @pl.when(jnp.logical_or(n == 1, n == 3))
        def _():
            hear(n // 2)
            greet(n // 2 + 1)

        return carry

    with jax.named_scope("prepare"):
        prepare()
    with jax.named_scope("scores"):
        lax.fori_loop(1, NZ + 1, scores_step, 0)
        hear(2)

    def spread(row):
        for r in range(ROWS // LANES):
            wide[r * LANES : (r + 1) * LANES, :] = jnp.broadcast_to(row[r : r + 1, :], (LANES, LANES)).T

    def plane_copies(phase):
        slot = row_buf.at[phase, me]
        ways = sorted(
            ((dx, dy) for dx in range(4) for dy in range(4) if dx or dy),
            key=lambda d: -min(d[0], 4 - d[0]) - min(d[1], 4 - d[1]),
        )
        return [
            copy(slot, slot, row_send.at[phase], row_recv.at[phase], same_rows(*d)) for d in ways
        ]

    def plane_bytes(phase):
        return bytes_of(row_buf.at[phase, pl.ds(0, NP - 1)], row_send.at[phase], row_recv.at[phase])

    def across_plane(phase, meanwhile):
        for c in plane_copies(phase):
            c.start()
        meanwhile()

        plane_bytes(phase).wait_recv()

    def plane_sent(phase):
        plane_bytes(phase).wait_send()

    QUAD = 4
    TALL = 256

    def quads(core_of):
        return [core_of * NZ + q * QUAD for q in range(NZ // QUAD)]

    def pick(x, k, h):
        return x[8 * k : 8 * k + 8, h * LANES : (h + 1) * LANES]

    def summed(op, xs):
        return op(functools.reduce(op, xs[0::2]), functools.reduce(op, xs[1::2])) if len(xs) > 1 else xs[0]

    def column_pass(first, into, held, term, op, start):
        def some(r, total):
            at = pl.ds(pl.multiple_of(r * TALL, TALL), TALL)
            w = wide.at[at, :]
            result = []
            for q in range(QUAD):
                view = held.at[first + q, at, :]
                for h in range(2):
                    xs = [term(pick(view, k, h), w[8 * k : 8 * k + 8, :]) for k in range(TALL // 8)]
                    result.append(op(total[2 * q + h], summed(op, xs)))
            return tuple(result)

        total = lax.fori_loop(0, ROWS // TALL, some, (jnp.full((8, LANES), start, F32),) * (2 * QUAD))
        fold = jnp.max if op is jnp.maximum else jnp.sum
        for c in range(2 * QUAD):
            into[pl.ds(2 * first + c, 1), :] = fold(total[c], axis=0, keepdims=True)

    def exp_pass(first):
        tall = 256

        def some(r, total):
            at = pl.ds(pl.multiple_of(r * tall, tall), tall)
            w = wide[at, :]
            result = []
            for q in range(QUAD):
                view = tile.at[first + q, at, :]
                out = kern.at[first + q, at, :]
                for h in range(2):
                    low = gamma[pl.ds(2 * (first + q) + h, 1), :]
                    entry = jnp.exp2((view[:, h * LANES : (h + 1) * LANES] + w) - low)
                    out[:, h * LANES : (h + 1) * LANES] = entry
                    result.append(total[2 * q + h] + jnp.sum(entry.reshape(tall // 8, 8, LANES), axis=0))
            return tuple(result)

        total = lax.fori_loop(0, ROWS // tall, some, (jnp.zeros((8, LANES), F32),) * (2 * QUAD))
        for c in range(2 * QUAD):
            col_stat[pl.ds(2 * first + c, 1), :] = jnp.sum(total[c], axis=0, keepdims=True)

    def row_pass(first, fresh):
        v = [weight[pl.ds(2 * first + c, 1), :] for c in range(2 * QUAD)]

        def some(r, carry):
            at = pl.ds(pl.multiple_of(r * TALL, TALL), TALL)
            views = [kern.at[first + q, at, :] for q in range(QUAD)]
            out = acc.at[at, :]
            for k in range(TALL // 8):
                total = summed(jnp.add, [pick(views[c // 2], k, c % 2) * v[c] for c in range(2 * QUAD)])
                out[8 * k : 8 * k + 8, :] = total if fresh else out[8 * k : 8 * k + 8, :] + total
            return carry

        lax.fori_loop(0, ROWS // TALL, some, 0)

    def halves(step):
        return pl.ds(pl.multiple_of(step * BLOCKS, BLOCKS), BLOCKS)

    def quad_rows(first):
        return pl.ds(pl.multiple_of(2 * first, 8), 8)

    def with_pair(phase, columns, emit):
        swaps_out = []
        for q, first in enumerate(quads(1 - core)):
            columns(first)
            rows = quad_rows(first)
            col_stat[rows, :] = gamma[rows, :] + jnp.log2(col_stat[rows, :])
            to = pair_buf.at[phase, pl.ds(8 * q, 8), :]
            k = 2 * phase + q
            swaps_out.append(copy(col_stat.at[rows, :], to, pair_send.at[k], pair_recv.at[k], pair))
            swaps_out[q].start()
        for q, first in enumerate(quads(core)):
            columns(first)
            rows = quad_rows(first)
            part = gamma[rows, :] + jnp.log2(col_stat[rows, :])
            swaps_out[q].wait()
            emit(q, lse2([part, pair_buf[phase, 8 * q : 8 * q + 8, :]]))

    def ring_copies(q):
        part = z_buf.at[z, pl.ds(8 * q, 8), :]
        return [
            copy(part, part, z_send.at[q], z_recv.at[q], on_ring(lax.rem(z + k, NZ))) for k in (4, 3, 5, 2, 6, 1, 7)
        ]

    def ring_bytes(phase):
        others = pl.ds(0, NZ - 1)
        ref = fin_buf.at[others] if phase == 2 else z_buf.at[others, pl.ds(0, 8), :]
        return bytes_of(ref, z_send.at[phase], z_recv.at[phase])

    with jax.named_scope("row_lse"):
        for r in range(ROWS // LANES):
            at = slice(r * LANES, (r + 1) * LANES)
            lane_top = top[at, :].T
            high = jnp.max(lane_top, axis=0, keepdims=True)
            total = jnp.sum(acc[at, :].T * jnp.exp2(lane_top - high), axis=0, keepdims=True)
            row_buf[0, me, r : r + 1, :] = high + jnp.log2(total)

    def after_gather():
        for r in range(ROWS // LANES):
            rows = rows_in[r * LANES : (r + 1) * LANES, :]
            row_stat[r : r + 1, :] = jnp.sum((rows * rows).T, axis=0, keepdims=True)

        @pl.when(carrier)
        def _():
            bytes_of(blocks.at[pl.ds(0, 14)], ring_send, d2d_recv.at[0]).wait_send()
            bytes_of(blocks.at[pl.ds(0, 15)], d2d_send, d2d_recv.at[0]).wait_send()

        @pl.when(jnp.logical_not(carrier))
        def _():
            pair_copy(z, 0).wait_send()

    with jax.named_scope("plane_0"):
        across_plane(0, after_gather)
    with jax.named_scope("spread"):
        phi = -log_dst - lse2([row_buf[0, q] for q in range(NP)])
        spread(phi)

    def first_columns(first):
        column_pass(first, gamma, tile, jnp.add, jnp.maximum, -jnp.inf)
        exp_pass(first)

    def to_ring(q, joined):
        z_buf[z, 8 * q : 8 * q + 8, :] = joined
        for c in ring_copies(q):
            c.start()

    with jax.named_scope("exp"):
        with_pair(0, first_columns, to_ring)
    with jax.named_scope("ring_0"):
        for q in range(2):
            ring_bytes(q).wait_recv()
    delta[halves(core), :] = -log_src - lse2([z_buf[k] for k in range(NZ)])
    half = delta.at[halves(core), :]
    give = copy(half, half, pair_send.at[4], pair_recv.at[4], pair)
    give.start()

    def weigh(core_of):
        rows = halves(core_of)
        weight[rows, :] = jnp.exp2(delta[rows, :] + gamma[rows, :])

    with jax.named_scope("rows_own"):
        weigh(core)
        for n, first in enumerate(quads(core)):
            row_pass(first, n == 0)
    with jax.named_scope("give"):
        give.wait()
    with jax.named_scope("rows_pair"):
        weigh(1 - core)
        for first in quads(1 - core):
            row_pass(first, False)
        for r in range(ROWS // LANES):
            at = slice(r * LANES, (r + 1) * LANES)
            row_buf[1, me, r : r + 1, :] = jnp.sum(acc[at, :].T, axis=0, keepdims=True)

    def after_ring():
        plane_sent(0)
        for q in range(2):
            ring_bytes(q).wait_send()

    with jax.named_scope("plane_1"):
        across_plane(1, after_ring)
    with jax.named_scope("spread"):
        log_sum = log_dst + jnp.log2(jnp.sum(row_buf[1], axis=0))
        spread(jnp.exp2(-log_sum))
        f_own[...] = row_stat[...] + (phi - log_sum) / SCALE
    hand = copy(f_own, f_pair, pair_send.at[5], pair_recv.at[5], pair)
    hand.start()

    def part_copy(to):
        return copy(own_buf.at[to], fin_buf.at[z], z_send.at[2], z_recv.at[2], on_ring(to))

    def to_owners(q, joined):
        for i in range(NZ // 2):
            to = NZ // 2 * q + i
            part = joined[2 * i : 2 * i + 2, :]
            own_buf[to] = part

            @pl.when(z == to)
            def _():
                fin_buf[to] = part

            @pl.when(z != to)
            def _():
                part_copy(to).start()

    with jax.named_scope("cols"):
        with_pair(1, lambda first: column_pass(first, col_stat, kern, jnp.multiply, jnp.add, 0.0), to_owners)
    with jax.named_scope("ring_1"):
        plane_sent(1)
        hand.wait()
        f_ref[...] = jnp.where(swaps, f_pair[...], f_own[...])
        ring_bytes(2).wait_recv()
    g_ref[...] = g0[...] - (log_src + lse2([fin_buf[k] for k in range(NZ)])) / SCALE
    ring_bytes(2).wait_send()


def body(sources, targets, duals_init):
    n_src = sources.shape[0] * lax.axis_size("blk")
    n_dst = targets.shape[0] * lax.axis_size("blk") * lax.axis_size("tgt")
    vmem = pl.BlockSpec(memory_space=pltpu.VMEM)
    dma = pltpu.SemaphoreType.DMA
    f, g = pl.pallas_call(
        functools.partial(kernel, math.log2(n_src), math.log2(n_dst)),
        out_shape=(pltpu.VMEM((8, LANES), F32), pltpu.VMEM((2, LANES), F32)),
        in_specs=[pl.BlockSpec(memory_space=pl.ANY)] * 3,
        out_specs=(vmem, vmem),
        scratch_shapes=[
            pltpu.VMEM((2, LANES), F32),
            dma((3,)),
            pltpu.VMEM((BLOCKS, ROWS, COLS), F32),
            pltpu.VMEM((BLOCKS, ROWS, COLS), F32),
            pltpu.VMEM((BLOCKS, HEAD + COLS, D), F32),
            pltpu.VMEM((ROWS, D), F32),
            pltpu.VMEM((ROWS, 4 * D), jnp.bfloat16),
            pltpu.VMEM((ROWS, LANES), F32),
            pltpu.VMEM((ROWS, LANES), F32),
            pltpu.VMEM((ROWS, LANES), F32),
            pltpu.VMEM((8, LANES), F32),
            pltpu.VMEM((2 * BLOCKS, LANES), F32),
            pltpu.VMEM((2 * BLOCKS, LANES), F32),
            pltpu.VMEM((2 * BLOCKS, LANES), F32),
            pltpu.VMEM((2 * BLOCKS, LANES), F32),
            pltpu.VMEM((2, NP, 8, LANES), F32),
            pltpu.VMEM((2, BLOCKS, LANES), F32),
            pltpu.VMEM((NZ, BLOCKS, LANES), F32),
            pltpu.VMEM((NZ, 2, LANES), F32),
            pltpu.VMEM((NZ, 2, LANES), F32),
            pltpu.VMEM((8, LANES), F32),
            pltpu.VMEM((8, LANES), F32),
            pltpu.SemaphoreType.REGULAR((3,)), dma, dma((2, 14)), dma, dma((NZ,)), dma((2,)), dma((2,)),
            dma((2,)), dma((2,)), dma((3,)), dma((3,)), dma((6,)), dma((6,)),
        ],
        compiler_params=pltpu.CompilerParams(
            collective_id=0, has_side_effects=True, vmem_limit_bytes=60 * 1024 * 1024
        ),
        name="sinkhorn",
    )(sources, targets, duals_init.reshape(2, LANES))
    return f.reshape(-1), g.reshape(-1)


def solution(mesh):
    return jax.shard_map(
        body,
        mesh=mesh,
        in_specs=(P("blk", None), P(("blk", "tgt"), None), P(("blk", "tgt"))),
        out_specs=(P("blk"), P(("blk", "tgt"))),
        check_vma=False,
    )
```

```python
import functools
import math

import jax
import jax.numpy as jnp
from jax import lax
from jax.experimental import pallas as pl
from jax.experimental.pallas import tpu as pltpu
from jax.sharding import PartitionSpec as P

EPS = 0.05
LOG2E = math.log2(math.e)
SCALE = LOG2E / EPS
MESH = pl.DeviceIdType.MESH
NZ = 8
NP = 16
ROWS = 1024
COLS = 256
BLOCKS = 16
HEAD = 8
D = 128
LANES = 128
CHUNK = 128
CUTS = ((0, HEAD + CHUNK), (HEAD + CHUNK, CHUNK))
F32 = jnp.float32


def lse2(parts):
    high = functools.reduce(jnp.maximum, parts)
    total = functools.reduce(jnp.add, [jnp.exp2(p - high) for p in parts])
    return high + jnp.log2(total)


def kernel(
    log_src, log_dst,
    src_ref, tgt_ref, g0_ref, f_ref, g_ref,
    g0, load_sem, stage, tile, kern, blocks, rows_in, lhs, acc, wide,
    top, row_stat, col_stat, gamma, delta, weight,
    row_buf, pair_buf, z_buf, own_buf, fin_buf, f_own, f_pair,
    met, ring_send, ring_recv, d2d_send, d2d_recv, x_send, x_recv,
    row_send, row_recv, z_send, z_recv, pair_send, pair_recv,
):
    blk, tgt = lax.axis_index("blk"), lax.axis_index("tgt")
    x_lo, z = blk // NZ, lax.rem(blk, NZ)
    core, x_hi, y = lax.rem(tgt, 2), lax.rem(tgt // 2, 2), tgt // 4
    pair = (blk, tgt + 1 - 2 * core)
    me = x_lo * 8 + tgt // 2

    x_at = 2 * x_hi + x_lo

    def off_plane(dx, dy):
        x, row = lax.rem(x_at + dx, 4), lax.rem(y + dy, 4)
        return lax.rem(x, 2) * NZ + z, row * 4 + (x // 2) * 2 + core

    def same_rows(dx, dy):
        blk_there, tgt_there = off_plane(dx, dy)
        return blk_there, tgt_there if dx % 2 == 0 else tgt_there + 1 - 2 * core

    def on_ring(other):
        return x_lo * NZ + other, tgt

    carrier = core == 1
    swaps = core == 0
    left, right = off_plane(3, 0), off_plane(1, 0)
    own = core * NZ + z

    loads = [
        pltpu.make_async_copy(tgt_ref, blocks.at[own, pl.ds(HEAD, COLS), :], load_sem.at[0]),
        pltpu.make_async_copy(g0_ref, g0, load_sem.at[1]),
        pltpu.make_async_copy(src_ref, rows_in, load_sem.at[2]),
        pltpu.make_async_copy(src_ref, stage, load_sem.at[2]),
    ]
    loads[0].start()
    loads[1].start()

    @pl.when(swaps)
    def _():
        loads[3].start()

    barrier = pltpu.get_barrier_semaphore()
    around = [off_plane(dx, dy) for dx, dy in ((1, 0), (3, 0), (0, 1), (0, 3))]
    for there in (on_ring(lax.rem(z + 1, NZ)), on_ring(lax.rem(z + NZ - 1, NZ)), pair, *around):
        pl.semaphore_signal(barrier, inc=1, device_id=there, device_id_type=MESH)

    @pl.when(jnp.logical_not(swaps))
    def _():
        loads[2].start()

    loads[0].wait()
    loads[1].wait()
    for half in range(2):
        part = blocks[own, HEAD + half * LANES : HEAD + (half + 1) * LANES, :]
        norm = jnp.sum((part * part).T, axis=0, keepdims=True)
        blocks[own, half : half + 1, :] = SCALE * (g0[half : half + 1, :] - norm)

    with jax.named_scope("barrier"):
        pl.semaphore_wait(barrier, 7)

    def copy(src, dst, send, recv, where):
        return pltpu.make_async_remote_copy(
            src_ref=src, dst_ref=dst, send_sem=send, recv_sem=recv, device_id=where, device_id_type=MESH
        )

    def piece(zb, i):
        start, size = CUTS[i % 2]
        return blocks.at[(NZ if i < 2 else 0) + zb, pl.ds(start, size), :]

    def ring_copy(way, step, i, zb):
        to = on_ring(lax.rem(z + (1 if way == 0 else NZ - 1), NZ))
        slot = 4 * (step - 1) + (i if step < 4 else i // 2)
        return copy(piece(zb, i), piece(zb, i), ring_send, ring_recv.at[way, slot], to)

    def pair_copy(zb, of):
        whole = blocks.at[of * NZ + zb]
        return copy(whole, whole, d2d_send, d2d_recv.at[zb], pair)

    def bytes_of(ref, send, recv):
        return copy(ref, ref, send, recv, pair)

    def goes(way, step, i):
        return step < 4 or i % 2 == way

    def swap_copy(side):
        at = pl.ds(side * (ROWS // 2), ROWS // 2)
        return copy(stage.at[at, :], rows_in.at[at, :], x_send.at[side], x_recv.at[side], (left, right)[side])

    @pl.when(jnp.logical_not(carrier))
    def _():
        pair_copy(z, 0).start()

    @pl.when(carrier)
    def _():
        for i in (0, 1):
            for way in range(2):
                ring_copy(way, 1, i, z).start()
        pair_copy(z, 1).start()

    @pl.when(swaps)
    def _():
        loads[3].wait()
        for side in range(2):
            swap_copy(side).start()

    @pl.when(carrier)
    def _():
        pair_copy(z, 0).wait_recv()
        for i in (2, 3):
            for way in range(2):
                ring_copy(way, 1, i, z).start()

    def greet(r):
        for there in around:
            pl.semaphore_signal(met.at[r], inc=1, device_id=there, device_id_type=MESH)

    def hear(r):
        pl.semaphore_wait(met.at[r], len(around))

    greet(0)

    def origin(way, step):
        return lax.rem(z + (NZ - step if way == 0 else step), NZ)

    def receive(step, half):
        @pl.when(carrier)
        def _():
            for i in range(2):
                start, size = CUTS[i]
                for way in range(2):
                    zb = origin(way, step)
                    part = blocks.at[(1 - half) * NZ + zb, pl.ds(start, size), :]
                    to = on_ring(lax.rem(z + (1 if way == 0 else NZ - 1), NZ))
                    slot = 4 * (step - 1) + 2 * half + i
                    came = copy(part, part, ring_send, ring_recv.at[way, slot], to)
                    came.wait_recv()
                    last = step == 3
                    slot = jnp.where(last, 12 + half, slot + 4)

                    @pl.when(jnp.logical_or(jnp.logical_not(last), i == way))
                    def _():
                        copy(part, part, ring_send, ring_recv.at[way, slot], to).start()

            for way in range(2):
                pair_copy(origin(way, step), 1 - half).start()

    def receive_far():
        @pl.when(carrier)
        def _():
            far = origin(0, 4)
            for half in range(2):
                for way in range(2):
                    ring_copy(way, 4, 2 * half + way, far).wait_recv()
                pair_copy(far, 1 - half).start()

    def prepare():
        @pl.when(swaps)
        def _():
            for side in range(2):
                swap_copy(side).wait()

        @pl.when(jnp.logical_not(swaps))
        def _():
            loads[2].wait()

        for r in range(ROWS // LANES):
            rows = rows_in[r * LANES : (r + 1) * LANES, :] * (2 * SCALE)
            high = rows.astype(jnp.bfloat16)
            low = (rows - high.astype(F32)).astype(jnp.bfloat16)
            lhs[r * LANES : (r + 1) * LANES, :] = jnp.concatenate([high, low, high, low], axis=1)
        top[...] = jnp.full_like(top, -jnp.inf)
        acc[...] = jnp.zeros_like(acc)

    def scores(zb):
        outs, heads, at = [], [], []
        for which in (core, 1 - core):
            b = which * NZ + zb
            t = blocks[b, HEAD:, :]
            high = t.astype(jnp.bfloat16)
            low = (t - high.astype(F32)).astype(jnp.bfloat16)
            rhs = jnp.concatenate([high, high, low, low], axis=1)
            outs.append(lax.dot_general(lhs[...], rhs, (((1,), (1,)), ((), ())), preferred_element_type=F32))
            heads += [jnp.broadcast_to(blocks[b, h : h + 1, :], (8, LANES)) for h in range(2)]
            at.append(b)
        for k in range(0, ROWS, 8):
            rows = slice(k, k + 8)
            parts = []
            for c in range(4):
                cut = slice((c % 2) * LANES, (c % 2 + 1) * LANES)
                parts.append(outs[c // 2][rows, cut] + heads[c])
                tile[at[c // 2], rows, cut] = parts[c]
            old = top[rows, :]
            new = jnp.maximum(jnp.maximum(parts[0], parts[1]), jnp.maximum(parts[2], parts[3]))
            new = jnp.maximum(old, new)
            top[rows, :] = new
            e = [jnp.exp2(p - new) for p in parts]
            acc[rows, :] = acc[rows, :] * jnp.exp2(old - new) + ((e[0] + e[1]) + (e[2] + e[3]))

    def scores_step(n, carry):
        half = lax.rem(n, 2)

        @pl.when(n == 2)
        def _():
            receive(1, 0)
            receive(1, 1)

        @pl.when(jnp.logical_and(n >= 3, n < 7))
        def _():
            receive((n + 1) // 2, 1 - half)

        @pl.when(n == NZ)
        def _():
            receive_far()

        off = n // 2
        zb = lax.rem(z + jnp.where(half == 0, NZ - off, off), NZ)

        @pl.when(jnp.logical_and(jnp.logical_not(carrier), n == 1))
        def _():
            pair_copy(z, 1).wait_recv()

        @pl.when(jnp.logical_and(jnp.logical_not(carrier), n > 1))
        def _():
            bytes_of(blocks.at[pl.ds(0, 2)], d2d_send, d2d_recv.at[zb]).wait_recv()

        scores(zb)

        @pl.when(jnp.logical_or(n == 1, n == 3))
        def _():
            hear(n // 2)
            greet(n // 2 + 1)

        return carry

    with jax.named_scope("prepare"):
        prepare()
    with jax.named_scope("scores"):
        lax.fori_loop(1, NZ + 1, scores_step, 0)
        hear(2)

    def spread(row):
        for r in range(ROWS // LANES):
            wide[r * LANES : (r + 1) * LANES, :] = jnp.broadcast_to(row[r : r + 1, :], (LANES, LANES)).T

    def plane_copies(phase):
        slot = row_buf.at[phase, me]
        ways = sorted(
            ((dx, dy) for dx in range(4) for dy in range(4) if dx or dy),
            key=lambda d: -min(d[0], 4 - d[0]) - min(d[1], 4 - d[1]),
        )
        return [
            copy(slot, slot, row_send.at[phase], row_recv.at[phase], same_rows(*d)) for d in ways
        ]

    def plane_bytes(phase):
        return bytes_of(row_buf.at[phase, pl.ds(0, NP - 1)], row_send.at[phase], row_recv.at[phase])

    def across_plane(phase, meanwhile):
        for c in plane_copies(phase):
            c.start()
        meanwhile()

        plane_bytes(phase).wait_recv()

    def plane_sent(phase):
        plane_bytes(phase).wait_send()

    QUAD = 4
    TALL = 256

    def quads(core_of):
        return [core_of * NZ + q * QUAD for q in range(NZ // QUAD)]

    def pick(x, k, h):
        return x[8 * k : 8 * k + 8, h * LANES : (h + 1) * LANES]

    def summed(op, xs):
        return op(functools.reduce(op, xs[0::2]), functools.reduce(op, xs[1::2])) if len(xs) > 1 else xs[0]

    def column_pass(first, into, held, term, op, start):
        def some(r, total):
            at = pl.ds(pl.multiple_of(r * TALL, TALL), TALL)
            w = wide.at[at, :]
            result = []
            for q in range(QUAD):
                view = held.at[first + q, at, :]
                for h in range(2):
                    xs = [term(pick(view, k, h), w[8 * k : 8 * k + 8, :]) for k in range(TALL // 8)]
                    result.append(op(total[2 * q + h], summed(op, xs)))
            return tuple(result)

        total = lax.fori_loop(0, ROWS // TALL, some, (jnp.full((8, LANES), start, F32),) * (2 * QUAD))
        fold = jnp.max if op is jnp.maximum else jnp.sum
        for c in range(2 * QUAD):
            into[pl.ds(2 * first + c, 1), :] = fold(total[c], axis=0, keepdims=True)

    def exp_pass(first):
        tall = 256

        def some(r, total):
            at = pl.ds(pl.multiple_of(r * tall, tall), tall)
            w = wide[at, :]
            result = []
            for q in range(QUAD):
                view = tile.at[first + q, at, :]
                out = kern.at[first + q, at, :]
                for h in range(2):
                    low = gamma[pl.ds(2 * (first + q) + h, 1), :]
                    entry = jnp.exp2((view[:, h * LANES : (h + 1) * LANES] + w) - low)
                    out[:, h * LANES : (h + 1) * LANES] = entry
                    result.append(total[2 * q + h] + jnp.sum(entry.reshape(tall // 8, 8, LANES), axis=0))
            return tuple(result)

        total = lax.fori_loop(0, ROWS // tall, some, (jnp.zeros((8, LANES), F32),) * (2 * QUAD))
        for c in range(2 * QUAD):
            col_stat[pl.ds(2 * first + c, 1), :] = jnp.sum(total[c], axis=0, keepdims=True)

    def row_pass(first, fresh):
        v = [weight[pl.ds(2 * first + c, 1), :] for c in range(2 * QUAD)]

        def some(r, carry):
            at = pl.ds(pl.multiple_of(r * TALL, TALL), TALL)
            views = [kern.at[first + q, at, :] for q in range(QUAD)]
            out = acc.at[at, :]
            for k in range(TALL // 8):
                total = summed(jnp.add, [pick(views[c // 2], k, c % 2) * v[c] for c in range(2 * QUAD)])
                out[8 * k : 8 * k + 8, :] = total if fresh else out[8 * k : 8 * k + 8, :] + total
            return carry

        lax.fori_loop(0, ROWS // TALL, some, 0)

    def halves(step):
        return pl.ds(pl.multiple_of(step * BLOCKS, BLOCKS), BLOCKS)

    def quad_rows(first):
        return pl.ds(pl.multiple_of(2 * first, 8), 8)

    def with_pair(phase, columns, emit):
        swaps_out = []
        for q, first in enumerate(quads(1 - core)):
            columns(first)
            rows = quad_rows(first)
            col_stat[rows, :] = gamma[rows, :] + jnp.log2(col_stat[rows, :])
            to = pair_buf.at[phase, pl.ds(8 * q, 8), :]
            k = 2 * phase + q
            swaps_out.append(copy(col_stat.at[rows, :], to, pair_send.at[k], pair_recv.at[k], pair))
            swaps_out[q].start()
        for q, first in enumerate(quads(core)):
            columns(first)
            rows = quad_rows(first)
            part = gamma[rows, :] + jnp.log2(col_stat[rows, :])
            swaps_out[q].wait()
            emit(q, lse2([part, pair_buf[phase, 8 * q : 8 * q + 8, :]]))

    def ring_copies(q):
        part = z_buf.at[z, pl.ds(8 * q, 8), :]
        return [
            copy(part, part, z_send.at[q], z_recv.at[q], on_ring(lax.rem(z + k, NZ))) for k in (4, 3, 5, 2, 6, 1, 7)
        ]

    def ring_bytes(phase):
        others = pl.ds(0, NZ - 1)
        ref = fin_buf.at[others] if phase == 2 else z_buf.at[others, pl.ds(0, 8), :]
        return bytes_of(ref, z_send.at[phase], z_recv.at[phase])

    with jax.named_scope("row_lse"):
        for r in range(ROWS // LANES):
            at = slice(r * LANES, (r + 1) * LANES)
            lane_top = top[at, :].T
            high = jnp.max(lane_top, axis=0, keepdims=True)
            total = jnp.sum(acc[at, :].T * jnp.exp2(lane_top - high), axis=0, keepdims=True)
            row_buf[0, me, r : r + 1, :] = high + jnp.log2(total)

    def after_gather():
        for r in range(ROWS // LANES):
            rows = rows_in[r * LANES : (r + 1) * LANES, :]
            row_stat[r : r + 1, :] = jnp.sum((rows * rows).T, axis=0, keepdims=True)

        @pl.when(carrier)
        def _():
            bytes_of(blocks.at[pl.ds(0, 14)], ring_send, d2d_recv.at[0]).wait_send()
            bytes_of(blocks.at[pl.ds(0, 15)], d2d_send, d2d_recv.at[0]).wait_send()

        @pl.when(jnp.logical_not(carrier))
        def _():
            pair_copy(z, 0).wait_send()

    with jax.named_scope("plane_0"):
        across_plane(0, after_gather)
    with jax.named_scope("spread"):
        phi = -log_dst - lse2([row_buf[0, q] for q in range(NP)])
        spread(phi)

    def first_columns(first):
        column_pass(first, gamma, tile, jnp.add, jnp.maximum, -jnp.inf)
        exp_pass(first)

    def to_ring(q, joined):
        z_buf[z, 8 * q : 8 * q + 8, :] = joined
        for c in ring_copies(q):
            c.start()

    with jax.named_scope("exp"):
        with_pair(0, first_columns, to_ring)
    with jax.named_scope("ring_0"):
        for q in range(2):
            ring_bytes(q).wait_recv()
    delta[halves(core), :] = -log_src - lse2([z_buf[k] for k in range(NZ)])
    half = delta.at[halves(core), :]
    give = copy(half, half, pair_send.at[4], pair_recv.at[4], pair)
    give.start()

    def weigh(core_of):
        rows = halves(core_of)
        weight[rows, :] = jnp.exp2(delta[rows, :] + gamma[rows, :])

    with jax.named_scope("rows_own"):
        weigh(core)
        for n, first in enumerate(quads(core)):
            row_pass(first, n == 0)
    with jax.named_scope("give"):
        give.wait()
    with jax.named_scope("rows_pair"):
        weigh(1 - core)
        for first in quads(1 - core):
            row_pass(first, False)
        for r in range(ROWS // LANES):
            at = slice(r * LANES, (r + 1) * LANES)
            row_buf[1, me, r : r + 1, :] = jnp.sum(acc[at, :].T, axis=0, keepdims=True)

    def after_ring():
        plane_sent(0)
        for q in range(2):
            ring_bytes(q).wait_send()

    with jax.named_scope("plane_1"):
        across_plane(1, after_ring)
    with jax.named_scope("spread"):
        log_sum = log_dst + jnp.log2(jnp.sum(row_buf[1], axis=0))
        spread(jnp.exp2(-log_sum))
        f_own[...] = row_stat[...] + (phi - log_sum) / SCALE
    hand = copy(f_own, f_pair, pair_send.at[5], pair_recv.at[5], pair)
    hand.start()

    def part_copy(to):
        return copy(own_buf.at[to], fin_buf.at[z], z_send.at[2], z_recv.at[2], on_ring(to))

    def to_owners(q, joined):
        for i in range(NZ // 2):
            to = NZ // 2 * q + i
            part = joined[2 * i : 2 * i + 2, :]
            own_buf[to] = part

            @pl.when(z == to)
            def _():
                fin_buf[to] = part

            @pl.when(z != to)
            def _():
                part_copy(to).start()

    with jax.named_scope("cols"):
        with_pair(1, lambda first: column_pass(first, col_stat, kern, jnp.multiply, jnp.add, 0.0), to_owners)
    with jax.named_scope("ring_1"):
        plane_sent(1)
        hand.wait()
        f_ref[...] = jnp.where(swaps, f_pair[...], f_own[...])
        ring_bytes(2).wait_recv()
    g_ref[...] = g0[...] - (log_src + lse2([fin_buf[k] for k in range(NZ)])) / SCALE
    ring_bytes(2).wait_send()


def body(sources, targets, duals_init):
    n_src = sources.shape[0] * lax.axis_size("blk")
    n_dst = targets.shape[0] * lax.axis_size("blk") * lax.axis_size("tgt")
    vmem = pl.BlockSpec(memory_space=pltpu.VMEM)
    dma = pltpu.SemaphoreType.DMA
    f, g = pl.pallas_call(
        functools.partial(kernel, math.log2(n_src), math.log2(n_dst)),
        out_shape=(pltpu.VMEM((8, LANES), F32), pltpu.VMEM((2, LANES), F32)),
        in_specs=[pl.BlockSpec(memory_space=pl.ANY)] * 3,
        out_specs=(vmem, vmem),
        scratch_shapes=[
            pltpu.VMEM((2, LANES), F32),
            dma((3,)),
            pltpu.VMEM((ROWS, D), F32),
            pltpu.VMEM((BLOCKS, ROWS, COLS), F32),
            pltpu.VMEM((BLOCKS, ROWS, COLS), F32),
            pltpu.VMEM((BLOCKS, HEAD + COLS, D), F32),
            pltpu.VMEM((ROWS, D), F32),
            pltpu.VMEM((ROWS, 4 * D), jnp.bfloat16),
            pltpu.VMEM((ROWS, LANES), F32),
            pltpu.VMEM((ROWS, LANES), F32),
            pltpu.VMEM((ROWS, LANES), F32),
            pltpu.VMEM((8, LANES), F32),
            pltpu.VMEM((2 * BLOCKS, LANES), F32),
            pltpu.VMEM((2 * BLOCKS, LANES), F32),
            pltpu.VMEM((2 * BLOCKS, LANES), F32),
            pltpu.VMEM((2 * BLOCKS, LANES), F32),
            pltpu.VMEM((2, NP, 8, LANES), F32),
            pltpu.VMEM((2, BLOCKS, LANES), F32),
            pltpu.VMEM((NZ, BLOCKS, LANES), F32),
            pltpu.VMEM((NZ, 2, LANES), F32),
            pltpu.VMEM((NZ, 2, LANES), F32),
            pltpu.VMEM((8, LANES), F32),
            pltpu.VMEM((8, LANES), F32),
            pltpu.SemaphoreType.REGULAR((3,)), dma, dma((2, 14)), dma, dma((NZ,)), dma((2,)), dma((2,)),
            dma((2,)), dma((2,)), dma((3,)), dma((3,)), dma((6,)), dma((6,)),
        ],
        compiler_params=pltpu.CompilerParams(
            collective_id=0, has_side_effects=True, vmem_limit_bytes=60 * 1024 * 1024
        ),
        name="sinkhorn",
    )(sources, targets, duals_init.reshape(2, LANES))
    return f.reshape(-1), g.reshape(-1)


def solution(mesh):
    return jax.shard_map(
        body,
        mesh=mesh,
        in_specs=(P("blk", None), P(("blk", "tgt"), None), P(("blk", "tgt"))),
        out_specs=(P("blk"), P(("blk", "tgt"))),
        check_vma=False,
    )
```
